256 devices in a mesh: gx: 8 (over x, core), gy: 8 (over z), gz: 4 (over y).
Axes of the slice: x: 4, y: 4, z: 8, core: 2. Of those that a mesh axis runs over, the one named last changes fastest.
Arguments:
- particle_mass: float32 [8388608], P(('gx', 'gy', 'gz')), may hold values from 0.5 to 2
- particle_velocity: float32 [3, 8388608], P(None, ('gx', 'gy', 'gz')), may hold values from -6 to 6
- particle_affine: float32 [9, 8388608], P(None, ('gx', 'gy', 'gz')), may hold values from -6 to 6
- particle_cell: int32 [3, 8388608], P(None, ('gx', 'gy', 'gz')), may hold values from 0 to 13
- particle_fraction: int32 [3, 8388608], P(None, ('gx', 'gy', 'gz')), may hold values from 0 to 1023
- block_owner: int32 [16384, 1], P(('gx', 'gy', 'gz')), may hold values from 0 to 31; in each aligned block of 64 rows (0 to 63, 64 to 127, ...) at most 4 rows name the same one
- block_slot: int32 [16384], P(('gx', 'gy', 'gz')), may hold values from 0 to 15
- block_count: int32 [16384], P(('gx', 'gy', 'gz')), may hold values from 128 to 512
- cell_drag: float32 [4096, 4096], P(('gx', 'gy', 'gz')), may hold values from 0.5 to 2
Outputs:
- grid_velocity: float32 [4096, 3, 4096], P(('gx', 'gy', 'gz'))
- new_velocity: float32 [3, 8388608], P(None, ('gx', 'gy', 'gz'))
- new_affine: float32 [9, 8388608], P(None, ('gx', 'gy', 'gz'))
The draws below stay inside these ranges and needn't reach their ends.
Inputs may be any that keep to these rules, and one draw needn't show every extreme that they name: `block_owner`: owner index counted over the devices with the particle device's own gx index, in gy+gz order; among the rows of one device, no owner is named more than 4 times. `block_count`: slots at or beyond the count are absent. `particle_cell`: A particle's three stencil nodes lie inside its grid block.
All inputs are finite; a program needn't handle non-finite values.
Results may differ from the reference program's by a relative error of at most 0.0085.
Values may be sent and summed in bfloat16 or wider, within the bound.
No kernel may reach another device: no remote copies, remote signals or barrier semaphores. Data moves between devices by JAX's collectives and lax.ppermute only.
A program may use at most 128 MiB of HBM per device.

```python
import math
import jax
import jax.numpy as jnp
import numpy as np
from jax import lax

EDGE = 16
PB = 512
QUANT = 1024
BLK_DEV = 64
GROUP = 32
CAP = 4
TILES_DEV = 16
BLOCKS = 16384
PARTICLES = 8388608
TILES = 4096
CELLS = 4096
N_GY = 8
N_GZ = 4


def place_ends(entries, key, smallest, high):
    longest = entries.shape.index(max(entries.shape))
    spots = []
    for shift in (0, 1):
        where = [jax.random.randint(jax.random.fold_in(key, axis), (), 0, length) for axis, length in enumerate(entries.shape)]
        where[longest] = (where[longest] + shift) % entries.shape[longest]
        spots.append(tuple(where))
    return entries.at[spots[0]].set(smallest).at[spots[1]].set(high)


def block_levels(own_key, dims, shards, low, largest):
    def one(axis_at, blocks):
        heights = jax.random.uniform(jax.random.fold_in(jax.random.fold_in(own_key, 6), axis_at), (blocks,), jnp.float32, low / len(shards), largest / len(shards))
        return jnp.repeat(jnp.exp(heights), dims[axis_at] // blocks).reshape((-1,) + (1,) * (len(dims) - axis_at - 1))

    loudness = one(*shards[0])
    for cut in shards[1:]:
        loudness = loudness * one(*cut)
    return loudness


def shared_out(stream_key, own, number, rows, amount, top, most, slope):
    order = jax.random.permutation(stream_key, amount)
    packed, common = load_shares(amount, rows * top, most, slope, True), load_shares(amount, rows * top, most, slope, False)
    places = jnp.arange(amount)

    def named(lengths, rotation):
        used = int((lengths > 0).sum())
        fixed = max(1, used // 4)
        shifted = fixed + (places - fixed + rotation * (used - fixed)) % max(1, amount - fixed)
        return jnp.zeros((amount,), jnp.int32).at[order[jnp.where(places < fixed, places, shifted)]].set(jnp.asarray(lengths, jnp.int32))

    lengths = jnp.where(number % 4 == 0, named(packed, number // 4), named(common, number - number // 4 - 1))
    mixed = jax.random.permutation(jax.random.fold_in(own, 3), amount)
    giver, receiver = mixed[0:amount // 2 * 2:2], mixed[1:amount // 2 * 2:2]
    margin = jnp.minimum(lengths[giver] - 1, most - lengths[receiver]) // 2
    margin = jnp.where((giver == order[0]) | (receiver == order[0]) | (lengths[receiver] == 0), 0, jnp.maximum(margin, 0))
    shifted = jax.random.randint(jax.random.fold_in(own, 4), (amount // 2,), 0, 1 << 20) % (margin + 1)
    lengths = lengths.at[giver].add(-shifted).at[receiver].add(shifted)
    labels = jnp.searchsorted(jnp.cumsum(lengths), jnp.arange(rows * top), side="right").astype(jnp.int32)
    table = labels.reshape(top, rows).T
    table = table[jax.random.permutation(jax.random.fold_in(own, 1), rows)]
    rotation = jax.random.randint(jax.random.fold_in(own, 2), (rows, 1), 0, top)
    return jnp.take_along_axis(table, (jnp.arange(top)[None, :] + rotation) % top, axis=1)


def load_shares(amount, total, bound, slope, full):
    loads = [(1 << 20) // math.isqrt(standing ** slope) + 1 for standing in range(1, amount + 1)]
    largest = bound if full else min(bound, max(-(-total // amount), total * loads[0] // sum(loads)))
    least = 1 if total - largest >= amount - 1 else 0
    holding, rest = [largest] + [least] * (amount - 1), total - largest - least * (amount - 1)
    while rest > 0:
        free = [i for i in range(1, amount) if holding[i] < largest] or [i for i in range(1, amount) if holding[i] < bound]
        whole, budget = sum([loads[i] for i in free]), rest
        for i in free:
            more = min(bound - holding[i], max(1, budget * loads[i] // whole), rest)
            holding[i] = holding[i] + more
            rest = rest - more
    return np.array(holding)


def gaussian(stream_key, extent, deviation, reach, pieces=(), kind=jnp.bfloat16):
    result = deviation * jax.random.normal(stream_key, extent, jnp.float32)
    if pieces:
        result = result * block_levels(stream_key, extent, pieces, -0.22, 0.18)
    return jnp.clip(result, -reach, reach).astype(kind)


def setup_inputs(seed: int = 0) -> dict:
    keys = jax.random.split(jax.random.key(seed), 10)
    particle_mass = jnp.clip(jnp.exp(math.log(2.0) - 1.3862944 * jax.random.uniform(keys[0], (PARTICLES,), jnp.float32) ** block_levels(keys[0], (PARTICLES,), ((0, 256),), -0.2, 0.2)), 0.5, 2.0)
    particle_velocity = gaussian(keys[1], (3, PARTICLES), 1.0, 6.0, ((1, 256),), jnp.float32)
    particle_affine = gaussian(keys[2], (9, PARTICLES), 1.0, 6.0, ((1, 256),), jnp.float32)
    particle_cell = place_ends(jax.random.randint(keys[3], (3, PARTICLES), 0, EDGE - 2), jax.random.fold_in(keys[3], 1), 0, (EDGE - 2) - 1).astype(jnp.int32)
    particle_fraction = place_ends(jax.random.randint(keys[4], (3, PARTICLES), 0, QUANT), jax.random.fold_in(keys[4], 1), 0, QUANT - 1).astype(jnp.int32)
    block_owner_keys = jax.random.split(jax.random.fold_in(keys[5], 1), BLOCKS // BLK_DEV)
    block_owner_turns = jax.random.permutation(jax.random.fold_in(keys[5], 3), BLOCKS // BLK_DEV)
    block_owner = jax.vmap(lambda own, number: shared_out(jax.random.fold_in(keys[5], 2), own, number, BLK_DEV, GROUP, 1, CAP, 2))(block_owner_keys, block_owner_turns).reshape((BLOCKS, 1))
    block_slot = place_ends(jax.random.randint(keys[6], (BLOCKS,), 0, TILES_DEV), jax.random.fold_in(keys[6], 1), 0, TILES_DEV - 1).astype(jnp.int32)
    block_count = place_ends(jax.random.randint(keys[7], (BLOCKS,), PB // 4, PB + 1), jax.random.fold_in(keys[7], 1), PB // 4, PB).astype(jnp.int32)
    cell_drag = jnp.clip(jnp.exp(math.log(2.0) - 1.3862944 * jax.random.uniform(keys[8], (TILES, CELLS), jnp.float32) ** block_levels(keys[8], (TILES, CELLS), ((0, 256),), -0.2, 0.2)), 0.5, 2.0)
    return dict(particle_mass=particle_mass, particle_velocity=particle_velocity, particle_affine=particle_affine, particle_cell=particle_cell, particle_fraction=particle_fraction, block_owner=block_owner, block_slot=block_slot, block_count=block_count, cell_drag=cell_drag)


def spline(offset):
    magnitude = jnp.abs(offset)
    inner_part = 0.75 - magnitude * magnitude
    outer_part = 0.5 * (1.5 - magnitude) * (1.5 - magnitude)
    return jnp.where(magnitude < 0.5, inner_part, jnp.where(magnitude < 1.5, outer_part, 0.0))


def particle_table(particle_mass, particle_velocity, particle_affine, particle_cell, particle_fraction, block_count):
    blocks = block_count.shape[0]
    batch_shape = (blocks, particle_mass.shape[0] // blocks)
    places = jnp.arange(batch_shape[1], dtype=jnp.int32)
    present = places[None, :] < block_count[:, None]
    live_mass = jnp.where(present, particle_mass.reshape(batch_shape), 0.0)
    position = particle_cell.astype(jnp.float32) + 0.5 + (particle_fraction.astype(jnp.float32) + 0.5) / QUANT
    return jnp.concatenate([live_mass[None], particle_velocity.reshape((3,) + batch_shape), particle_affine.reshape((9,) + batch_shape), position.reshape((3,) + batch_shape)], axis=0)


def stencil(particle_data):
    node_coords = jnp.arange(EDGE, dtype=jnp.float32)
    offset = node_coords[None, :, None, None] - particle_data[13:16][:, None]
    weights = spline(offset)
    return weights, weights * offset


def planes(weights, slopes):
    def outer(first_factor, second_factor):
        product_table = first_factor[:, None] * second_factor[None, :]
        return product_table.reshape((EDGE * EDGE,) + product_table.shape[2:]).astype(jnp.bfloat16)
    return outer(weights[1], weights[2]), outer(slopes[1], weights[2]), outer(weights[1], slopes[2])


def deposit(particle_data):
    batch_shape = particle_data.shape[1:]
    weights, slopes = stencil(particle_data)
    plane_zero, plane_one, plane_two = planes(weights, slopes)
    live_mass = particle_data[0]
    along_x = weights[0]
    slope_x = slopes[0]
    affine = particle_data[4:13].reshape((3, 3) + batch_shape)
    mass_lead = (live_mass[None] * along_x)[None]
    momentum_lead = live_mass[None, None] * (particle_data[1:4][:, None] * along_x[None] + affine[:, 0][:, None] * slope_x[None])
    lead_zero = jnp.concatenate([mass_lead, momentum_lead], axis=0).astype(jnp.bfloat16)
    lead_one = (live_mass[None, None] * affine[:, 1][:, None] * along_x[None]).astype(jnp.bfloat16)
    lead_two = (live_mass[None, None] * affine[:, 2][:, None] * along_x[None]).astype(jnp.bfloat16)

    def contract(lead, plane):
        flattened = lead.reshape((-1,) + batch_shape).astype(jnp.float32)
        return jnp.einsum("anp,bnp->nab", flattened, plane.astype(jnp.float32), precision=lax.Precision.HIGHEST)

    count_blocks = batch_shape[0]
    dep_zero = contract(lead_zero, plane_zero).reshape(count_blocks, 4, -1)
    dep_one = contract(lead_one, plane_one).reshape(count_blocks, 3, -1)
    dep_two = contract(lead_two, plane_two).reshape(count_blocks, 3, -1)
    return jnp.concatenate([dep_zero[:, :1], dep_zero[:, 1:] + dep_one + dep_two], axis=1)


def interpolate(particle_data, grid_rows):
    batch_shape = particle_data.shape[1:]
    weights, slopes = stencil(particle_data)
    plane_zero, plane_one, plane_two = planes(weights, slopes)
    along_x = weights[0]
    slope_x = slopes[0]
    flattened = grid_rows.reshape(batch_shape[0], 3 * EDGE, EDGE * EDGE).astype(jnp.float32)

    def contract(plane):
        moment = jnp.einsum("nab,bnp->anp", flattened, plane.astype(jnp.float32), precision=lax.Precision.HIGHEST)
        return moment.reshape((3, EDGE) + batch_shape)

    moment_zero = contract(plane_zero)
    moment_one = contract(plane_one)
    moment_two = contract(plane_two)
    velocity_out = jnp.sum(along_x[None] * moment_zero, axis=1)
    column_zero = 4.0 * jnp.sum(slope_x[None] * moment_zero, axis=1)
    column_one = 4.0 * jnp.sum(along_x[None] * moment_one, axis=1)
    column_two = 4.0 * jnp.sum(along_x[None] * moment_two, axis=1)
    affine_out = jnp.stack([column_zero, column_one, column_two], axis=1).reshape((9,) + batch_shape)
    present = (particle_data[0] > 0.0).astype(jnp.float32)
    return jnp.concatenate([velocity_out, affine_out], axis=0) * present[None]


def reference(particle_mass, particle_velocity, particle_affine, particle_cell, particle_fraction, block_owner, block_slot, block_count, cell_drag):
    group_size = N_GY * N_GZ
    particle_data = particle_table(particle_mass, particle_velocity, particle_affine, particle_cell, particle_fraction, block_count)
    blocks = block_count.shape[0]
    device = jnp.arange(blocks, dtype=jnp.int32) // BLK_DEV
    tile_ids = (((device // group_size) * group_size + block_owner[:, 0]) * TILES_DEV + block_slot).astype(jnp.int32)

    def accumulate(grid_sums, block_index):
        portion = lax.dynamic_slice_in_dim(particle_data, block_index, 1, 1)
        return grid_sums.at[tile_ids[block_index]].add(deposit(portion)[0]), None

    initial = jnp.zeros((cell_drag.shape[0], 4, cell_drag.shape[1]), jnp.float32)
    grid_sums = lax.scan(accumulate, initial, jnp.arange(blocks, dtype=jnp.int32))[0]
    grid_velocity = grid_sums[:, 1:] / (grid_sums[:, :1] + cell_drag[:, None, :])
    rounded = grid_velocity.astype(jnp.bfloat16)

    def sample(block_index):
        portion = lax.dynamic_slice_in_dim(particle_data, block_index, 1, 1)
        cell_rows = lax.dynamic_index_in_dim(rounded, tile_ids[block_index], 0, keepdims=True)
        return interpolate(portion, cell_rows)[:, 0]

    finished = lax.map(sample, jnp.arange(blocks, dtype=jnp.int32))
    finished = jnp.transpose(finished, (1, 0, 2)).reshape(12, -1)
    return grid_velocity, finished[:3], finished[3:]
```

```python
import functools

import jax
import jax.numpy as jnp
from jax import lax
from jax.experimental import pallas as pl
from jax.experimental.pallas import tpu as pltpu
from jax.sharding import PartitionSpec as P

EDGE = 16
PLANE = EDGE * EDGE
QUANT = 1024
LANES = 128
ROWS = 80
BACK = 48
CENTER = 7.5
SMEM = pltpu.SMEM
VMEM = pltpu.VMEM


def pack_kernel(
    owner_ref, tile_ref, mass_ref, vel_ref, aff_ref, cell_ref, frac_ref, out_ref, dest_ref, used_ref, scratch, *, capacity, group
):
    blocks = dest_ref.shape[0]
    length = vel_ref.shape[1] // blocks
    parts = length // LANES

    def clear(owner, carry):
        used_ref[owner] = 0
        for rank in range(capacity):
            first = pl.multiple_of((owner * capacity + rank) * ROWS, 16)
            out_ref[pl.ds(first, 16), :] = jnp.full((16, LANES), -1.0, jnp.bfloat16)
        return carry

    lax.fori_loop(0, group, clear, 0)

    def place(block):
        owner = owner_ref[block]
        rank = used_ref[owner]
        used_ref[owner] = rank + 1
        slot = owner * capacity + rank
        dest_ref[block] = slot
        return slot

    def move(block, slot, buffer):
        where = pl.ds(pl.multiple_of(block * length, LANES), length)
        code = cell_ref[:, where] * QUANT + frac_ref[:, where]
        high = code >> 7
        low = (code & 127).astype(jnp.float32)
        buffer[0:9, :] = aff_ref[:, where]
        buffer[9:12, :] = vel_ref[:, where]
        buffer[12:15, :] = high.astype(jnp.float32)
        buffer[15:16, :] = jnp.full((1, length), tile_ref[block], jnp.int32).astype(jnp.float32)
        first = pl.multiple_of(slot * ROWS, 16)
        packed = buffer[...].astype(jnp.bfloat16)
        for part in range(parts):
            out_ref[pl.ds(pl.multiple_of(first + 16 * part, 16), 16), :] = packed[:, part * LANES : (part + 1) * LANES]
        pieces = [low[e : e + 1, part * LANES : (part + 1) * LANES] for e in range(3) for part in range(parts)]
        pieces.append(mass_ref[block])
        aux = jnp.concatenate(pieces, axis=0)
        out_ref[pl.ds(pl.multiple_of(first + 16 * parts, 16), 16), :] = aux.astype(jnp.bfloat16)

    def step(index, carry):
        slots = [place(index * 2 + k) for k in range(2)]
        for k in range(2):
            move(index * 2 + k, slots[k], scratch.at[k])
        return carry

    lax.fori_loop(0, blocks // 2, step, 0)


def node_weights(position):
    nodes = lax.broadcasted_iota(jnp.int32, (EDGE, position.shape[1]), 0).astype(jnp.float32)
    offset = nodes - position
    outer = jnp.maximum(1.5 - jnp.abs(offset), 0.0)
    inner = jnp.maximum(outer - 1.0, 0.0)
    return 0.5 * outer * outer - 1.5 * inner * inner, offset


def split(value):
    high = value.astype(jnp.bfloat16)
    return high, (value - high.astype(jnp.float32)).astype(jnp.bfloat16)


def particle_rows(data_ref, slot, parts):
    first = pl.multiple_of(slot * ROWS, 16)
    main = jnp.concatenate(
        [data_ref[pl.ds(pl.multiple_of(first + 16 * part, 16), 16), :] for part in range(parts)], axis=1
    ).astype(jnp.float32)
    aux = data_ref[pl.ds(pl.multiple_of(first + 16 * parts, 16), 16), :].astype(jnp.float32)

    def spread(row):
        return jnp.concatenate([aux[row * parts + part : row * parts + part + 1] for part in range(parts)], axis=1)

    positions = [main[12 + e : 13 + e] * 0.125 + (spread(e) * (1.0 / QUANT) + (0.5 + 0.5 / QUANT)) for e in range(3)]
    return main, spread(3), positions


def plane_table(weight_y, weight_z):
    return jnp.concatenate([(weight_y[y : y + 1] * weight_z).astype(jnp.bfloat16) for y in range(EDGE)], axis=0)


def deposit_block(data_ref, slot, parts):
    main, mass, (pos_x, pos_y, pos_z) = particle_rows(data_ref, slot, parts)
    weight_x, offset_x = node_weights(pos_x)
    weight_y, unused = node_weights(pos_y)
    weight_z, unused = node_weights(pos_z)
    plane = plane_table(weight_y, weight_z)
    center_y = pos_y - CENTER
    center_z = pos_z - CENTER
    loaded = mass * weight_x
    exact = [[], [], []]
    for d in range(3):
        column_zero, column_one, column_two = (main[3 * d + e : 3 * d + e + 1] for e in range(3))
        base = main[9 + d : 10 + d] - column_one * center_y - column_two * center_z
        exact[0].append(loaded * (base + column_zero * offset_x))
        exact[1].append(loaded * column_one)
        exact[2].append(loaded * column_two)
    halves = [split(value) for rows in exact for value in rows]
    lead = jnp.concatenate(
        [loaded.astype(jnp.bfloat16)] + [high for high, low in halves] + [low for high, low in halves], axis=0
    )
    sums = lax.dot_general(lead, plane, (((1,), (1,)), ((), ())), preferred_element_type=jnp.float32)
    momentum = sums[EDGE : 10 * EDGE] + sums[10 * EDGE :]
    return jnp.concatenate([sums[:EDGE], momentum], axis=0)


def interpolate_block(data_ref, grid_rows, slot, parts):
    unused, unused, (pos_x, pos_y, pos_z) = particle_rows(data_ref, slot, parts)
    weight_x, offset_x = node_weights(pos_x)
    weight_y, unused = node_weights(pos_y)
    weight_z, unused = node_weights(pos_z)
    plane = plane_table(weight_y, weight_z)
    moments = jnp.dot(grid_rows, plane, preferred_element_type=jnp.float32)
    span = 3 * EDGE
    moment_zero = moments[:span]
    moment_one = moments[span : 2 * span] + moments[2 * span : 3 * span]
    moment_two = moments[3 * span : 4 * span] + moments[4 * span :]
    center_y = pos_y - CENTER
    center_z = pos_z - CENTER

    def total(value):
        return jnp.sum(value, axis=0, keepdims=True)

    velocity, affine = [], []
    for d in range(3):
        rows = slice(d * EDGE, (d + 1) * EDGE)
        weighted = weight_x * moment_zero[rows]
        speed = total(weighted)
        velocity.append(speed)
        affine.append(4.0 * total(weighted * offset_x))
        affine.append(4.0 * (total(weight_x * moment_one[rows]) - center_y * speed))
        affine.append(4.0 * (total(weight_x * moment_two[rows]) - center_z * speed))
    return affine + velocity


def main_kernel(
    tile_ref, data_ref, drag_ref, back_ref, grid_ref, list_ref, sums_ref, rows_ref, scratch, *, parts
):
    slots = tile_ref.shape[0]
    tiles = drag_ref.shape[0]

    def collect(slot, count):
        @pl.when(tile_ref[slot] >= 0)
        def _():
            list_ref[count] = slot

        return count + (tile_ref[slot] >= 0).astype(jnp.int32)

    count = lax.fori_loop(0, slots, collect, 0)
    pairs = (count + 1) // 2

    def clear(tile, carry):
        sums_ref[tile] = jnp.zeros(sums_ref.shape[1:], jnp.float32)
        return carry

    lax.fori_loop(0, tiles, clear, 0)

    def second_of(pair):
        return list_ref[jnp.minimum(2 * pair + 1, count - 1)]

    def deposit_pair(pair, carry):
        first = list_ref[2 * pair]
        second = second_of(pair)
        spare = jnp.where(2 * pair + 1 < count, tile_ref[second], tiles)
        one = deposit_block(data_ref, first, parts)
        two = deposit_block(data_ref, second, parts)
        tile = tile_ref[first]
        sums_ref[tile] = sums_ref[tile] + one
        sums_ref[spare] = sums_ref[spare] + two
        return carry

    lax.fori_loop(0, pairs, deposit_pair, 0)

    lane = lax.broadcasted_iota(jnp.int32, (EDGE, PLANE), 1)
    node_y = (lane >> 4).astype(jnp.float32) - CENTER
    node_z = (lane & 15).astype(jnp.float32) - CENTER

    def update(tile, carry):
        sums = sums_ref[tile]
        weight = sums[:EDGE] + drag_ref[tile]
        ones, twos, zeros = [], [], []
        for d in range(3):
            zero, one, two = (sums[EDGE * (1 + 3 * e + d) : EDGE * (2 + 3 * e + d)] for e in range(3))
            speed = (zero + node_y * one + node_z * two) / weight
            grid_ref[tile, d] = speed
            rounded = speed.astype(jnp.bfloat16)
            zeros.append(rounded)
            ones.append(split(rounded.astype(jnp.float32) * node_y))
            twos.append(split(rounded.astype(jnp.float32) * node_z))
        rows = zeros + [high for high, low in ones] + [low for high, low in ones]
        rows = rows + [high for high, low in twos] + [low for high, low in twos]
        rows_ref[tile] = jnp.concatenate(rows, axis=0)
        return carry

    lax.fori_loop(0, tiles, update, 0)

    def send(values, slot, buffer):
        for row, value in enumerate(values):
            for part in range(parts):
                at = part * 8 + row if row < 8 else 8 * parts + part * 4 + row - 8
                buffer[at : at + 1, :] = value[:, part * LANES : (part + 1) * LANES]
        back_ref[pl.ds(pl.multiple_of(slot * BACK, 16), BACK), :] = buffer[...].astype(jnp.bfloat16)

    def interpolate_pair(pair, carry):
        first = list_ref[2 * pair]
        second = second_of(pair)
        one = interpolate_block(data_ref, rows_ref[tile_ref[first]], first, parts)
        two = interpolate_block(data_ref, rows_ref[tile_ref[second]], second, parts)
        send(one, first, scratch.at[0])
        send(two, second, scratch.at[1])
        return carry

    lax.fori_loop(0, pairs, interpolate_pair, 0)


def unpack_kernel(dest_ref, count_ref, back_ref, vel_ref, aff_ref):
    blocks = dest_ref.shape[0]
    length = vel_ref.shape[1] // blocks
    parts = length // LANES

    def one(block):
        first = pl.multiple_of(dest_ref[block] * BACK, 16)
        rows = back_ref[pl.ds(first, BACK), :].astype(jnp.float32)
        for part in range(parts):
            lane = lax.broadcasted_iota(jnp.int32, (8, LANES), 1) + part * LANES
            present = lane < count_ref[block]
            where = pl.ds(pl.multiple_of(block * length + part * LANES, LANES), LANES)
            aff_ref[0:8, where] = jnp.where(present, rows[part * 8 : part * 8 + 8], 0.0)
            rest = jnp.where(present[:4], rows[8 * parts + part * 4 : 8 * parts + part * 4 + 4], 0.0)
            aff_ref[8:9, where] = rest[0:1]
            vel_ref[:, where] = rest[1:4]

    def step(index, carry):
        for k in range(2):
            one(index * 2 + k)
        return carry

    lax.fori_loop(0, blocks // 2, step, 0)


def per_device(
    particle_mass,
    particle_velocity,
    particle_affine,
    particle_cell,
    particle_fraction,
    block_owner,
    block_slot,
    block_count,
    cell_drag,
):
    group = lax.axis_size(("gy", "gz"))
    blocks = block_count.shape[0]
    particles = particle_mass.shape[0]
    capacity = max(1, 2 * blocks // group)
    slots = group * capacity
    tiles = cell_drag.shape[0]
    length = particles // blocks
    parts = length // LANES
    mass = particle_mass.reshape(blocks, parts, LANES)
    live = lax.broadcasted_iota(jnp.int32, mass.shape, 1) * LANES + lax.broadcasted_iota(jnp.int32, mass.shape, 2)
    mass = jnp.where(live < block_count[:, None, None], mass, 0.0)
    smem = pl.BlockSpec(memory_space=SMEM)
    vmem = pl.BlockSpec(memory_space=VMEM)
    outgoing, destination = pl.pallas_call(
        functools.partial(pack_kernel, capacity=capacity, group=group),
        out_shape=(
            jax.ShapeDtypeStruct((slots * ROWS, LANES), jnp.bfloat16),
            jax.ShapeDtypeStruct((blocks,), jnp.int32),
        ),
        in_specs=[smem, smem, vmem, vmem, vmem, vmem, vmem],
        out_specs=(vmem, smem),
        scratch_shapes=[SMEM((group,), jnp.int32), VMEM((2, 16, length), jnp.float32)],
        name="pack",
    )(block_owner.reshape(blocks), block_slot, mass, particle_velocity, particle_affine, particle_cell, particle_fraction)
    arrived = lax.all_to_all(outgoing, ("gy", "gz"), split_axis=0, concat_axis=0, tiled=True)
    tile_ids = arrived.reshape(slots, ROWS, LANES)[:, 15, 0].astype(jnp.int32)
    span = 3 * EDGE
    back, grid = pl.pallas_call(
        functools.partial(main_kernel, parts=parts),
        out_shape=(
            jax.ShapeDtypeStruct((slots * BACK, LANES), jnp.bfloat16),
            jax.ShapeDtypeStruct((tiles, 3, EDGE, PLANE), jnp.float32),
        ),
        in_specs=[smem, vmem, vmem],
        out_specs=(vmem, vmem),
        scratch_shapes=[
            SMEM((slots,), jnp.int32),
            VMEM((tiles + 1, 10 * EDGE, PLANE), jnp.float32),
            VMEM((tiles, 5 * span, PLANE), jnp.bfloat16),
            VMEM((2, BACK, LANES), jnp.float32),
        ],
        name="transfer",
    )(tile_ids, arrived, cell_drag.reshape(tiles, EDGE, PLANE))
    returned = lax.all_to_all(back, ("gy", "gz"), split_axis=0, concat_axis=0, tiled=True)
    new_velocity, new_affine = pl.pallas_call(
        unpack_kernel,
        out_shape=(
            jax.ShapeDtypeStruct((3, particles), jnp.float32),
            jax.ShapeDtypeStruct((9, particles), jnp.float32),
        ),
        in_specs=[smem, smem, vmem],
        out_specs=(vmem, vmem),
        name="unpack",
    )(destination, block_count, returned)
    return (grid.reshape(tiles, 3, EDGE * PLANE), new_velocity, new_affine)


def solution(mesh):
    whole = ("gx", "gy", "gz")
    return jax.shard_map(
        per_device,
        mesh=mesh,
        in_specs=(
            P(whole),
            P(None, whole),
            P(None, whole),
            P(None, whole),
            P(None, whole),
            P(whole, None),
            P(whole),
            P(whole),
            P(whole, None),
        ),
        out_specs=(P(whole, None, None), P(None, whole), P(None, whole)),
        check_vma=False,
    )
```

```python
import functools

import jax
import jax.numpy as jnp
from jax import lax
from jax.experimental import pallas as pl
from jax.experimental.pallas import tpu as pltpu
from jax.sharding import PartitionSpec as P

EDGE = 16
PLANE = EDGE * EDGE
QUANT = 1024
LANES = 128
ROWS = 80
BACK = 48
CENTER = 7.5
SMEM = pltpu.SMEM
VMEM = pltpu.VMEM


def pack_kernel(
    owner_ref,
    tile_ref,
    count_ref,
    mass_ref,
    vel_ref,
    aff_ref,
    cell_ref,
    frac_ref,
    out_ref,
    dest_ref,
    used_ref,
    scratch,
    *,
    capacity,
    group,
):
    half = capacity // 2
    blocks = dest_ref.shape[0]
    length = vel_ref.shape[1] // blocks
    parts = length // LANES

    def slot_of(owner, rank):
        return (rank // half) * (group * half) + owner * half + rank % half

    def clear(owner, carry):
        used_ref[owner] = 0
        for rank in range(capacity):
            first = pl.multiple_of(slot_of(owner, rank) * ROWS, 16)
            out_ref[pl.ds(first, 16), :] = jnp.full((16, LANES), -1.0, jnp.bfloat16)
        return carry

    lax.fori_loop(0, group, clear, 0)

    def place(block):
        owner = owner_ref[block]
        rank = used_ref[owner]
        used_ref[owner] = rank + 1
        slot = slot_of(owner, rank)
        dest_ref[block] = slot
        return slot

    def move(block, slot, buffer):
        where = pl.ds(pl.multiple_of(block * length, LANES), length)
        code = cell_ref[:, where] * QUANT + frac_ref[:, where]
        high = code >> 7
        low = (code & 127).astype(jnp.float32)
        buffer[0:9, :] = aff_ref[:, where]
        buffer[9:12, :] = vel_ref[:, where]
        buffer[12:15, :] = high.astype(jnp.float32)
        buffer[15:16, :] = jnp.full((1, length), tile_ref[block], jnp.int32).astype(jnp.float32)
        first = pl.multiple_of(slot * ROWS, 16)
        packed = buffer[...].astype(jnp.bfloat16)
        for part in range(parts):
            out_ref[pl.ds(pl.multiple_of(first + 16 * part, 16), 16), :] = packed[:, part * LANES : (part + 1) * LANES]
        pieces = [low[e : e + 1, part * LANES : (part + 1) * LANES] for e in range(3) for part in range(parts)]
        place_in_block = lax.broadcasted_iota(jnp.int32, (parts, LANES), 0) * LANES
        place_in_block = place_in_block + lax.broadcasted_iota(jnp.int32, (parts, LANES), 1)
        pieces.append(jnp.where(place_in_block < count_ref[block], mass_ref[block], 0.0))
        aux = jnp.concatenate(pieces, axis=0)
        out_ref[pl.ds(pl.multiple_of(first + 16 * parts, 16), 16), :] = aux.astype(jnp.bfloat16)

    def step(index, carry):
        slots = [place(index * 2 + k) for k in range(2)]
        for k in range(2):
            move(index * 2 + k, slots[k], scratch.at[k])
        return carry

    lax.fori_loop(0, blocks // 2, step, 0)


def node_weights(position):
    nodes = lax.broadcasted_iota(jnp.int32, (EDGE, position.shape[1]), 0).astype(jnp.float32)
    offset = nodes - position
    outer = jnp.maximum(1.5 - jnp.abs(offset), 0.0)
    inner = jnp.maximum(outer - 1.0, 0.0)
    return 0.5 * outer * outer - 1.5 * inner * inner, offset


def split(value):
    high = value.astype(jnp.bfloat16)
    return high, (value - high.astype(jnp.float32)).astype(jnp.bfloat16)


def particle_rows(data_ref, slot, parts):
    first = pl.multiple_of(slot * ROWS, 16)
    main = jnp.concatenate(
        [data_ref[pl.ds(pl.multiple_of(first + 16 * part, 16), 16), :] for part in range(parts)], axis=1
    ).astype(jnp.float32)
    aux = data_ref[pl.ds(pl.multiple_of(first + 16 * parts, 16), 16), :].astype(jnp.float32)

    def spread(row):
        return jnp.concatenate([aux[row * parts + part : row * parts + part + 1] for part in range(parts)], axis=1)

    positions = [main[12 + e : 13 + e] * 0.125 + (spread(e) * (1.0 / QUANT) + (0.5 + 0.5 / QUANT)) for e in range(3)]
    return main, spread(3), positions


def plane_table(weight_y, weight_z):
    return jnp.concatenate([(weight_y[y : y + 1] * weight_z).astype(jnp.bfloat16) for y in range(EDGE)], axis=0)


def deposit_block(data_ref, slot, parts):
    main, mass, (pos_x, pos_y, pos_z) = particle_rows(data_ref, slot, parts)
    weight_x, offset_x = node_weights(pos_x)
    weight_y, unused = node_weights(pos_y)
    weight_z, unused = node_weights(pos_z)
    plane = plane_table(weight_y, weight_z)
    center_y = pos_y - CENTER
    center_z = pos_z - CENTER
    loaded = mass * weight_x
    exact = [[], [], []]
    for d in range(3):
        column_zero, column_one, column_two = (main[3 * d + e : 3 * d + e + 1] for e in range(3))
        base = main[9 + d : 10 + d] - column_one * center_y - column_two * center_z
        exact[0].append(loaded * (base + column_zero * offset_x))
        exact[1].append(loaded * column_one)
        exact[2].append(loaded * column_two)
    halves = [split(value) for rows in exact for value in rows]
    lead = jnp.concatenate(
        [loaded.astype(jnp.bfloat16)] + [high for high, low in halves] + [low for high, low in halves], axis=0
    )
    sums = lax.dot_general(lead, plane, (((1,), (1,)), ((), ())), preferred_element_type=jnp.float32)
    momentum = sums[EDGE : 10 * EDGE] + sums[10 * EDGE :]
    return jnp.concatenate([sums[:EDGE], momentum], axis=0)


def interpolate_block(data_ref, grid_rows, slot, parts):
    unused, unused, (pos_x, pos_y, pos_z) = particle_rows(data_ref, slot, parts)
    weight_x, offset_x = node_weights(pos_x)
    weight_y, unused = node_weights(pos_y)
    weight_z, unused = node_weights(pos_z)
    plane = plane_table(weight_y, weight_z)
    moments = jnp.dot(grid_rows, plane, preferred_element_type=jnp.float32)
    span = 3 * EDGE
    moment_zero = moments[:span]
    moment_one = moments[span : 2 * span] + moments[2 * span : 3 * span]
    moment_two = moments[3 * span : 4 * span] + moments[4 * span :]
    center_y = pos_y - CENTER
    center_z = pos_z - CENTER

    def total(value):
        return jnp.sum(value, axis=0, keepdims=True)

    velocity, affine = [], []
    for d in range(3):
        rows = slice(d * EDGE, (d + 1) * EDGE)
        weighted = weight_x * moment_zero[rows]
        speed = total(weighted)
        velocity.append(speed)
        affine.append(4.0 * total(weighted * offset_x))
        affine.append(4.0 * (total(weight_x * moment_one[rows]) - center_y * speed))
        affine.append(4.0 * (total(weight_x * moment_two[rows]) - center_z * speed))
    return affine + velocity


def arrivals(data_ref, row_ref, tile_ref, list_ref, sem):
    slots = row_ref.shape[0]

    def read(slot, carry):
        first = data_ref[pl.ds(pl.multiple_of(slot * ROWS, 16), 16), :].astype(jnp.float32)
        row_ref[pl.ds(slot, 1), :] = first[15:16].astype(jnp.int32)
        return carry

    lax.fori_loop(0, slots, read, 0, unroll=4)
    copy = pltpu.make_async_copy(row_ref, tile_ref, sem)
    copy.start()
    copy.wait()

    def collect(slot, count):
        filled = tile_ref[slot, 0] >= 0

        @pl.when(filled)
        def _():
            list_ref[count] = slot

        return count + filled.astype(jnp.int32)

    return lax.fori_loop(0, slots, collect, 0)


def pair_of(pair, count, list_ref, tile_ref, spare):
    first = list_ref[2 * pair]
    second = list_ref[jnp.minimum(2 * pair + 1, count - 1)]
    other = jnp.where(2 * pair + 1 < count, tile_ref[second, 0], spare)
    return first, second, tile_ref[first, 0], other


def deposit_all(data_ref, sums_ref, tile_ref, list_ref, count, parts):
    spare = sums_ref.shape[0] - 1

    def step(pair, carry):
        first, second, tile, other = pair_of(pair, count, list_ref, tile_ref, spare)
        one = deposit_block(data_ref, first, parts)
        two = deposit_block(data_ref, second, parts)
        sums_ref[tile] = sums_ref[tile] + one
        sums_ref[other] = sums_ref[other] + two
        return carry

    lax.fori_loop(0, (count + 1) // 2, step, 0)


def interpolate_all(data_ref, rows_ref, back_ref, scratch, tile_ref, list_ref, count, parts):
    def send(values, slot, buffer):
        for row, value in enumerate(values):
            for part in range(parts):
                at = part * 8 + row if row < 8 else 8 * parts + part * 4 + row - 8
                buffer[at : at + 1, :] = value[:, part * LANES : (part + 1) * LANES]
        back_ref[pl.ds(pl.multiple_of(slot * BACK, 16), BACK), :] = buffer[...].astype(jnp.bfloat16)

    def step(pair, carry):
        first, second, tile, unused = pair_of(pair, count, list_ref, tile_ref, 0)
        one = interpolate_block(data_ref, rows_ref[tile], first, parts)
        two = interpolate_block(data_ref, rows_ref[tile_ref[second, 0]], second, parts)
        send(one, first, scratch.at[0])
        send(two, second, scratch.at[1])
        return carry

    lax.fori_loop(0, (count + 1) // 2, step, 0)


def early_kernel(data_ref, sums_ref, row_ref, tile_ref, list_ref, sem, *, parts):
    count = arrivals(data_ref, row_ref, tile_ref, list_ref, sem)

    def clear(tile, carry):
        sums_ref[tile] = jnp.zeros(sums_ref.shape[1:], jnp.float32)
        return carry

    lax.fori_loop(0, sums_ref.shape[0], clear, 0)
    deposit_all(data_ref, sums_ref, tile_ref, list_ref, count, parts)


def middle_kernel(
    early_ref, late_ref, sums_ref, drag_ref, back_ref, grid_ref, rows_ref, row_ref, tile_ref, list_ref, scratch, sem, *, parts
):
    count = arrivals(late_ref, row_ref, tile_ref, list_ref, sem)
    deposit_all(late_ref, sums_ref, tile_ref, list_ref, count, parts)
    lane = lax.broadcasted_iota(jnp.int32, (EDGE, PLANE), 1)
    node_y = (lane >> 4).astype(jnp.float32) - CENTER
    node_z = (lane & 15).astype(jnp.float32) - CENTER

    def update(tile, carry):
        sums = sums_ref[tile]
        weight = sums[:EDGE] + drag_ref[tile]
        ones, twos, zeros = [], [], []
        for d in range(3):
            zero, one, two = (sums[EDGE * (1 + 3 * e + d) : EDGE * (2 + 3 * e + d)] for e in range(3))
            speed = (zero + node_y * one + node_z * two) / weight
            grid_ref[tile, d] = speed
            rounded = speed.astype(jnp.bfloat16)
            zeros.append(rounded)
            ones.append(split(rounded.astype(jnp.float32) * node_y))
            twos.append(split(rounded.astype(jnp.float32) * node_z))
        rows = zeros + [high for high, low in ones] + [low for high, low in ones]
        rows = rows + [high for high, low in twos] + [low for high, low in twos]
        rows_ref[tile] = jnp.concatenate(rows, axis=0)
        return carry

    lax.fori_loop(0, drag_ref.shape[0], update, 0)
    count = arrivals(early_ref, row_ref, tile_ref, list_ref, sem)
    interpolate_all(early_ref, rows_ref, back_ref, scratch, tile_ref, list_ref, count, parts)


def last_kernel(data_ref, rows_ref, back_ref, row_ref, tile_ref, list_ref, scratch, sem, *, parts):
    count = arrivals(data_ref, row_ref, tile_ref, list_ref, sem)
    interpolate_all(data_ref, rows_ref, back_ref, scratch, tile_ref, list_ref, count, parts)


def unpack_kernel(dest_ref, count_ref, early_ref, late_ref, vel_ref, aff_ref):
    blocks = dest_ref.shape[0]
    length = vel_ref.shape[1] // blocks
    parts = length // LANES
    half = early_ref.shape[0] // BACK

    def put(block, source, slot):
        rows = source[pl.ds(pl.multiple_of(slot * BACK, 16), BACK), :].astype(jnp.float32)
        for part in range(parts):
            lane = lax.broadcasted_iota(jnp.int32, (8, LANES), 1) + part * LANES
            present = lane < count_ref[block]
            where = pl.ds(pl.multiple_of(block * length + part * LANES, LANES), LANES)
            aff_ref[0:8, where] = jnp.where(present, rows[part * 8 : part * 8 + 8], 0.0)
            rest = jnp.where(present[:4], rows[8 * parts + part * 4 : 8 * parts + part * 4 + 4], 0.0)
            aff_ref[8:9, where] = rest[0:1]
            vel_ref[:, where] = rest[1:4]

    def step(block, carry):
        slot = dest_ref[block]

        @pl.when(slot < half)
        def _():
            put(block, early_ref, slot)

        @pl.when(slot >= half)
        def _():
            put(block, late_ref, slot - half)

        return carry

    lax.fori_loop(0, blocks, step, 0)


def per_device(
    particle_mass,
    particle_velocity,
    particle_affine,
    particle_cell,
    particle_fraction,
    block_owner,
    block_slot,
    block_count,
    cell_drag,
):
    group = lax.axis_size(("gy", "gz"))
    blocks = block_count.shape[0]
    particles = particle_mass.shape[0]
    capacity = max(1, 2 * blocks // group)
    slots = group * capacity
    tiles = cell_drag.shape[0]
    length = particles // blocks
    parts = length // LANES
    half = slots // 2
    smem = pl.BlockSpec(memory_space=SMEM)
    vmem = pl.BlockSpec(memory_space=VMEM)
    outgoing, destination = pl.pallas_call(
        functools.partial(pack_kernel, capacity=capacity, group=group),
        out_shape=(
            jax.ShapeDtypeStruct((slots * ROWS, LANES), jnp.bfloat16),
            jax.ShapeDtypeStruct((blocks,), jnp.int32),
        ),
        in_specs=[smem, smem, smem, vmem, vmem, vmem, vmem, vmem],
        out_specs=(vmem, smem),
        scratch_shapes=[SMEM((group,), jnp.int32), VMEM((2, 16, length), jnp.float32)],
        name="pack",
    )(
        block_owner.reshape(blocks),
        block_slot,
        block_count,
        particle_mass.reshape(blocks, parts, LANES),
        particle_velocity,
        particle_affine,
        particle_cell,
        particle_fraction,
    )

    def exchange(array):
        return lax.all_to_all(array, ("gy", "gz"), split_axis=0, concat_axis=0, tiled=True)

    early = exchange(outgoing[: half * ROWS])
    late = exchange(outgoing[half * ROWS :])
    span = 3 * EDGE
    back_shape = jax.ShapeDtypeStruct((half * BACK, LANES), jnp.bfloat16)
    rows_shape = jax.ShapeDtypeStruct((tiles, 5 * span, PLANE), jnp.bfloat16)
    listing = [VMEM((half, LANES), jnp.int32), SMEM((half, LANES), jnp.int32), SMEM((half,), jnp.int32)]
    buffers = VMEM((2, BACK, LANES), jnp.float32)
    done = pltpu.SemaphoreType.DMA
    sums = pl.pallas_call(
        functools.partial(early_kernel, parts=parts),
        out_shape=jax.ShapeDtypeStruct((tiles + 1, 10 * EDGE, PLANE), jnp.float32),
        in_specs=[vmem],
        out_specs=vmem,
        scratch_shapes=listing + [done],
        name="early",
    )(early)
    back_early, grid, rows = pl.pallas_call(
        functools.partial(middle_kernel, parts=parts),
        out_shape=(back_shape, jax.ShapeDtypeStruct((tiles, 3, EDGE, PLANE), jnp.float32), rows_shape),
        in_specs=[vmem, vmem, vmem, vmem],
        out_specs=(vmem, vmem, vmem),
        scratch_shapes=listing + [buffers, done],
        name="middle",
    )(early, late, sums, cell_drag.reshape(tiles, EDGE, PLANE))
    returned_early = exchange(back_early)
    back_late = pl.pallas_call(
        functools.partial(last_kernel, parts=parts),
        out_shape=back_shape,
        in_specs=[vmem, vmem],
        out_specs=vmem,
        scratch_shapes=listing + [buffers, done],
        name="last",
    )(late, rows)
    returned_late = exchange(back_late)
    new_velocity, new_affine = pl.pallas_call(
        unpack_kernel,
        out_shape=(
            jax.ShapeDtypeStruct((3, particles), jnp.float32),
            jax.ShapeDtypeStruct((9, particles), jnp.float32),
        ),
        in_specs=[smem, smem, vmem, vmem],
        out_specs=(vmem, vmem),
        name="unpack",
    )(destination, block_count, returned_early, returned_late)
    return (grid.reshape(tiles, 3, EDGE * PLANE), new_velocity, new_affine)


def solution(mesh):
    whole = ("gx", "gy", "gz")
    return jax.shard_map(
        per_device,
        mesh=mesh,
        in_specs=(
            P(whole),
            P(None, whole),
            P(None, whole),
            P(None, whole),
            P(None, whole),
            P(whole, None),
            P(whole),
            P(whole),
            P(whole, None),
        ),
        out_specs=(P(whole, None, None), P(None, whole), P(None, whole)),
        check_vma=False,
    )
```

```python
import functools

import jax
import jax.numpy as jnp
from jax import lax
from jax.experimental import pallas as pl
from jax.experimental.pallas import tpu as pltpu
from jax.sharding import PartitionSpec as P

EDGE = 16
PLANE = EDGE * EDGE
QUANT = 1024
LANES = 128
ROWS = 80
BACK = 48
CENTER = 7.5
SMEM = pltpu.SMEM
VMEM = pltpu.VMEM


def pack_kernel(
    owner_ref, tile_ref, count_ref, mass_ref, vel_ref, aff_ref, cell_ref, frac_ref, out_ref, dest_ref, used_ref, scratch, low_ref, *, capacity, group
):
    blocks = dest_ref.shape[0]
    length = vel_ref.shape[1] // blocks
    parts = length // LANES

    def clear(owner, carry):
        used_ref[owner] = 0
        for rank in range(capacity):
            first = pl.multiple_of((owner * capacity + rank) * ROWS, 16)
            out_ref[pl.ds(first, 16), :] = jnp.full((16, LANES), -1.0, jnp.bfloat16)
        return carry

    lax.fori_loop(0, group, clear, 0)

    def place(block):
        owner = owner_ref[block]
        rank = used_ref[owner]
        used_ref[owner] = rank + 1
        slot = owner * capacity + rank
        dest_ref[block] = slot
        return slot

    place_in_block = lax.broadcasted_iota(jnp.int32, (parts, LANES), 0) * LANES
    place_in_block = place_in_block + lax.broadcasted_iota(jnp.int32, (parts, LANES), 1)

    def move(block, slot, buffer, lows):
        where = pl.ds(pl.multiple_of(block * length, LANES), length)
        code = cell_ref[:, where] * QUANT + frac_ref[:, where]
        low = (code & 127).astype(jnp.float32)
        for d in range(3):
            buffer[d : d + 1, :] = aff_ref[3 * d + 1 : 3 * d + 2, where]
            buffer[8 + d : 9 + d, :] = aff_ref[3 * d + 2 : 3 * d + 3, where]
            buffer[3 + 4 * d : 4 + 4 * d, :] = aff_ref[3 * d : 3 * d + 1, where]
        buffer[4:7, :] = vel_ref[:, where]
        buffer[12:15, :] = (code >> 7).astype(jnp.float32)
        buffer[15:16, :] = jnp.full((1, length), tile_ref[block], jnp.int32).astype(jnp.float32)
        live = jnp.where(place_in_block < count_ref[block], mass_ref[block], 0.0)
        for part in range(parts):
            lows[4 * part : 4 * part + 3, :] = low[:, part * LANES : (part + 1) * LANES]
            lows[4 * part + 3 : 4 * part + 4, :] = live[part : part + 1]
        first = pl.multiple_of(slot * ROWS, 16)
        packed = buffer[...].astype(jnp.bfloat16)
        for part in range(parts):
            out_ref[pl.ds(pl.multiple_of(first + 16 * part, 16), 16), :] = packed[:, part * LANES : (part + 1) * LANES]
        out_ref[pl.ds(pl.multiple_of(first + 16 * parts, 16), 16), :] = lows[...].astype(jnp.bfloat16)

    def step(index, carry):
        slots = [place(index * 2 + k) for k in range(2)]
        for k in range(2):
            move(index * 2 + k, slots[k], scratch.at[k], low_ref.at[k])
        return carry

    lax.fori_loop(0, blocks // 2, step, 0)


def split(value):
    high = value.astype(jnp.bfloat16)
    return high, (value - high.astype(jnp.float32)).astype(jnp.bfloat16)


def sublanes():
    return lax.broadcasted_iota(jnp.int32, (8, LANES), 0)


def spread(ref, row):
    return ref[pl.ds(row, 8, stride=0), :]


CELL, FIRST, SECOND, THIRD, MIDDLE, SIDE, NODES = (64 + 16 * k for k in range(7))
BASE = NODES + 64
TABLE = BASE + 32


def prepare(data_ref, slot, table, parts, deposit):
    first = pl.multiple_of(slot * ROWS, 16)
    side = data_ref[pl.ds(pl.multiple_of(first + 16 * parts, 16), 16), :].astype(jnp.float32)
    highs = []
    for part in range(parts):
        main = data_ref[pl.ds(pl.multiple_of(first + 16 * part, 16), 16), :].astype(jnp.float32)
        if deposit:
            table[16 * part : 16 * part + 16, :] = main
        highs.append(main[8:])
    upper = sublanes() < 4
    high = jnp.concatenate(
        [jnp.where(upper, pltpu.roll(highs[k], 4, 0), highs[k + 1]) for k in range(0, parts, 2)], axis=0
    )
    high = high * 0.125
    cell = jnp.floor(high)
    inside = (high - cell) + (side * (1.0 / QUANT) + 0.5 / QUANT)
    rest = 1.0 - inside
    table[CELL : CELL + 16, :] = cell
    table[FIRST : FIRST + 16, :] = rest * rest
    table[SECOND : SECOND + 16, :] = 1.0 + 2.0 * (inside * rest)
    table[THIRD : THIRD + 16, :] = inside * inside
    table[MIDDLE : MIDDLE + 16, :] = cell + inside + (0.5 - CENTER)
    if deposit:
        table[SIDE : SIDE + 16, :] = side * 0.125


def node_weights(table, part, e, nodes):
    row = 4 * part + e
    cell = spread(table, CELL + row)
    one, two, three = (spread(table, at + row) for at in (FIRST, SECOND, THIRD))
    return [
        jnp.where(cell == node, one, jnp.where(cell == node - 1.0, two, jnp.where(cell == node - 2.0, three, 0.0)))
        for node in nodes
    ]


def plane_table(table, part, nodes):
    for half, weight in enumerate(node_weights(table, part, 1, nodes)):
        table[NODES + 16 * part + 8 * half : NODES + 16 * part + 8 * half + 8, :] = weight
    upper, lower = node_weights(table, part, 2, nodes)
    rows = []
    for y in range(EDGE):
        weight = spread(table, NODES + 16 * part + y)
        rows.append(jnp.concatenate([weight * upper, weight * lower], axis=0).astype(jnp.bfloat16))
    return jnp.concatenate(rows, axis=0)


def node_rows():
    node = sublanes().astype(jnp.float32)
    return [node, node + 8.0]


def deposit_block(data_ref, slot, table, parts):
    prepare(data_ref, slot, table, parts, True)
    nodes = node_rows()
    leads, planes = [], []
    for part in range(parts):
        planes.append(plane_table(table, part, nodes))
        row = 4 * part
        weights = node_weights(table, part, 0, nodes)
        middle = spread(table, MIDDLE + row)
        offsets = [(node - CENTER) - middle for node in nodes]
        mass = spread(table, SIDE + row + 3)
        loaded = [mass * weight for weight in weights]
        top = table[16 * part : 16 * part + 8, :]
        bottom = table[16 * part + 8 : 16 * part + 16, :]
        base = pltpu.roll(top, 4, 0) - top * spread(table, MIDDLE + row + 1) - bottom * spread(table, MIDDLE + row + 2)
        table[BASE + 8 * part : BASE + 8 * part + 8, :] = base
        highs, lows = [jnp.concatenate(loaded, axis=0).astype(jnp.bfloat16)], []

        def add(values):
            high, low = split(jnp.concatenate(values, axis=0))
            highs.append(high)
            lows.append(low)

        for d in range(3):
            shift = spread(table, BASE + 8 * part + d)
            along_x = spread(table, 16 * part + 3 + 4 * d)
            add([load * (shift + along_x * offset) for load, offset in zip(loaded, offsets)])
        for at in (0, 8):
            for d in range(3):
                column = spread(table, 16 * part + at + d)
                add([load * column for load in loaded])
        leads.append(jnp.concatenate(highs + lows, axis=0))
    lead = jnp.concatenate(leads, axis=1)
    plane = jnp.concatenate(planes, axis=1)
    sums = lax.dot_general(lead, plane, (((1,), (1,)), ((), ())), preferred_element_type=jnp.float32)
    momentum = sums[EDGE : 10 * EDGE] + sums[10 * EDGE :]
    return jnp.concatenate([sums[:EDGE], momentum], axis=0)


def fold(values):
    row = sublanes()
    for shift in (1, 2, 4):
        if len(values) == 1:
            return values[0] + pltpu.roll(values[0], 8 - shift, 0)
        mine = (row & shift) == 0
        values = [
            jnp.where(mine, one, two) + pltpu.roll(jnp.where(mine, two, one), 8 - shift, 0)
            for one, two in zip(values[0::2], values[1::2])
        ]
    return values[0]


def interpolate_block(data_ref, grid_rows, slot, table, back_ref, parts):
    prepare(data_ref, slot, table, parts, False)
    nodes = node_rows()
    plane = jnp.concatenate([plane_table(table, part, nodes) for part in range(parts)], axis=1)
    moments = jnp.dot(grid_rows, plane, preferred_element_type=jnp.float32)
    span = 3 * EDGE
    row = sublanes()
    eights, fours = [], []
    for part in range(parts):
        weights = node_weights(table, part, 0, nodes)
        middle = spread(table, MIDDLE + 4 * part)
        offsets = [(node - CENTER) - middle for node in nodes]
        lanes = slice(part * LANES, (part + 1) * LANES)
        zero, one, two, speed = [], [], [], []
        for d in range(3):
            halves = [d * EDGE, d * EDGE + 8]
            loaded = [weight * moments[at : at + 8, lanes] for weight, at in zip(weights, halves)]
            speed.append(loaded[0] + loaded[1])
            zero.append(loaded[0] * offsets[0] + loaded[1] * offsets[1])
            for first, into in ((span, one), (3 * span, two)):
                pieces = [
                    weight * (moments[first + at : first + at + 8, lanes] + moments[first + span + at : first + span + at + 8, lanes])
                    for weight, at in zip(weights, halves)
                ]
                into.append(pieces[0] + pieces[1])
        eight = fold([zero[0], one[0], two[0], zero[1], one[1], two[1], zero[2], one[2]])
        four = fold([two[2]] + speed)
        table[BASE + 8 * part : BASE + 8 * part + 8, :] = four
        speeds = [spread(table, BASE + 8 * part + 1 + d) for d in range(3)]
        center_y = spread(table, MIDDLE + 4 * part + 1)
        center_z = spread(table, MIDDLE + 4 * part + 2)
        column = row % 3
        center = jnp.where(column == 1, center_y, jnp.where(column == 2, center_z, 0.0))
        speed = jnp.where(row < 3, speeds[0], jnp.where(row < 6, speeds[1], speeds[2]))
        eights.append(0.5 * (eight - center * speed))
        fours.append(jnp.where((row & 3) == 0, 0.5 * (four - center_z * speeds[2]), 0.125 * four))
    first = pl.multiple_of(slot * BACK, 16)
    upper = row < 4
    merged = [jnp.where(upper, fours[k], fours[k + 1]) for k in range(0, parts, 2)]
    back_ref[pl.ds(first, BACK), :] = jnp.concatenate(eights + merged, axis=0).astype(jnp.bfloat16)


def arrivals(data_ref, row_ref, tile_ref, list_ref, sem):
    slots = row_ref.shape[0]

    def read(slot, carry):
        first = data_ref[pl.ds(pl.multiple_of(slot * ROWS, 16), 16), :].astype(jnp.float32)
        row_ref[pl.ds(slot, 1), :] = first[15:16].astype(jnp.int32)
        return carry

    lax.fori_loop(0, slots, read, 0, unroll=4)
    copy = pltpu.make_async_copy(row_ref, tile_ref, sem)
    copy.start()
    copy.wait()

    def collect(slot, count):
        filled = tile_ref[slot, 0] >= 0

        @pl.when(filled)
        def _():
            list_ref[count] = slot

        return count + filled.astype(jnp.int32)

    return lax.fori_loop(0, slots, collect, 0)


def main_kernel(
    data_ref, drag_ref, back_ref, grid_ref, row_ref, tile_ref, list_ref, sums_ref, rows_ref, table, sem, *, parts
):
    tiles = drag_ref.shape[0]
    count = arrivals(data_ref, row_ref, tile_ref, list_ref, sem)
    pairs = (count + 1) // 2

    def clear(tile, carry):
        sums_ref[tile] = jnp.zeros(sums_ref.shape[1:], jnp.float32)
        return carry

    lax.fori_loop(0, tiles, clear, 0)

    def second_of(pair):
        return list_ref[jnp.minimum(2 * pair + 1, count - 1)]

    def deposit_pair(pair, carry):
        first = list_ref[2 * pair]
        second = second_of(pair)
        spare = jnp.where(2 * pair + 1 < count, tile_ref[second, 0], tiles)
        one = deposit_block(data_ref, first, table.at[0], parts)
        two = deposit_block(data_ref, second, table.at[1], parts)
        tile = tile_ref[first, 0]
        sums_ref[tile] = sums_ref[tile] + one
        sums_ref[spare] = sums_ref[spare] + two
        return carry

    lax.fori_loop(0, pairs, deposit_pair, 0)

    lane = lax.broadcasted_iota(jnp.int32, (EDGE, PLANE), 1)
    node_y = (lane >> 4).astype(jnp.float32) - CENTER
    node_z = (lane & 15).astype(jnp.float32) - CENTER

    def update(tile, carry):
        sums = sums_ref[tile]
        weight = sums[:EDGE] + drag_ref[tile]
        ones, twos, zeros = [], [], []
        for d in range(3):
            zero, one, two = (sums[EDGE * (1 + 3 * e + d) : EDGE * (2 + 3 * e + d)] for e in range(3))
            speed = (zero + node_y * one + node_z * two) / weight
            grid_ref[tile, d] = speed
            rounded = speed.astype(jnp.bfloat16)
            zeros.append(rounded)
            ones.append(split(rounded.astype(jnp.float32) * node_y))
            twos.append(split(rounded.astype(jnp.float32) * node_z))
        rows = zeros + [high for high, low in ones] + [low for high, low in ones]
        rows = rows + [high for high, low in twos] + [low for high, low in twos]
        rows_ref[tile] = jnp.concatenate(rows, axis=0)
        return carry

    lax.fori_loop(0, tiles, update, 0)

    def interpolate_pair(pair, carry):
        first = list_ref[2 * pair]
        second = second_of(pair)
        interpolate_block(data_ref, rows_ref[tile_ref[first, 0]], first, table.at[0], back_ref, parts)
        interpolate_block(data_ref, rows_ref[tile_ref[second, 0]], second, table.at[1], back_ref, parts)
        return carry

    lax.fori_loop(0, pairs, interpolate_pair, 0)


def unpack_kernel(dest_ref, count_ref, back_ref, vel_ref, aff_ref):
    blocks = dest_ref.shape[0]
    length = vel_ref.shape[1] // blocks
    parts = length // LANES

    def one(block):
        first = pl.multiple_of(dest_ref[block] * BACK, 16)
        rows = back_ref[pl.ds(first, BACK), :].astype(jnp.float32)
        for part in range(parts):
            lane = lax.broadcasted_iota(jnp.int32, (8, LANES), 1) + part * LANES
            present = lane < count_ref[block]
            where = pl.ds(pl.multiple_of(block * length + part * LANES, LANES), LANES)
            aff_ref[0:8, where] = jnp.where(present, rows[part * 8 : part * 8 + 8], 0.0)
            rest = jnp.where(present[:4], rows[8 * parts + part * 4 : 8 * parts + part * 4 + 4], 0.0)
            aff_ref[8:9, where] = rest[0:1]
            vel_ref[:, where] = rest[1:4]

    def step(index, carry):
        for k in range(2):
            one(index * 2 + k)
        return carry

    lax.fori_loop(0, blocks // 2, step, 0)


def per_device(
    particle_mass,
    particle_velocity,
    particle_affine,
    particle_cell,
    particle_fraction,
    block_owner,
    block_slot,
    block_count,
    cell_drag,
):
    group = lax.axis_size(("gy", "gz"))
    blocks = block_count.shape[0]
    particles = particle_mass.shape[0]
    capacity = max(1, 2 * blocks // group)
    slots = group * capacity
    tiles = cell_drag.shape[0]
    length = particles // blocks
    parts = length // LANES
    smem = pl.BlockSpec(memory_space=SMEM)
    vmem = pl.BlockSpec(memory_space=VMEM)
    outgoing, destination = pl.pallas_call(
        functools.partial(pack_kernel, capacity=capacity, group=group),
        out_shape=(
            jax.ShapeDtypeStruct((slots * ROWS, LANES), jnp.bfloat16),
            jax.ShapeDtypeStruct((blocks,), jnp.int32),
        ),
        in_specs=[smem, smem, smem, vmem, vmem, vmem, vmem, vmem],
        out_specs=(vmem, smem),
        scratch_shapes=[
            SMEM((group,), jnp.int32),
            VMEM((2, 16, length), jnp.float32),
            VMEM((2, 16, LANES), jnp.float32),
        ],
        name="pack",
    )(
        block_owner.reshape(blocks),
        block_slot,
        block_count,
        particle_mass.reshape(blocks, parts, LANES),
        particle_velocity,
        particle_affine,
        particle_cell,
        particle_fraction,
    )
    arrived = lax.all_to_all(outgoing, ("gy", "gz"), split_axis=0, concat_axis=0, tiled=True)
    span = 3 * EDGE
    back, grid = pl.pallas_call(
        functools.partial(main_kernel, parts=parts),
        out_shape=(
            jax.ShapeDtypeStruct((slots * BACK, LANES), jnp.bfloat16),
            jax.ShapeDtypeStruct((tiles, 3, EDGE, PLANE), jnp.float32),
        ),
        in_specs=[vmem, vmem],
        out_specs=(vmem, vmem),
        scratch_shapes=[
            VMEM((slots, LANES), jnp.int32),
            SMEM((slots, LANES), jnp.int32),
            SMEM((slots,), jnp.int32),
            VMEM((tiles + 1, 10 * EDGE, PLANE), jnp.float32),
            VMEM((tiles, 5 * span, PLANE), jnp.bfloat16),
            VMEM((2, TABLE, LANES), jnp.float32),
            pltpu.SemaphoreType.DMA,
        ],
        name="transfer",
    )(arrived, cell_drag.reshape(tiles, EDGE, PLANE))
    returned = lax.all_to_all(back, ("gy", "gz"), split_axis=0, concat_axis=0, tiled=True)
    new_velocity, new_affine = pl.pallas_call(
        unpack_kernel,
        out_shape=(
            jax.ShapeDtypeStruct((3, particles), jnp.float32),
            jax.ShapeDtypeStruct((9, particles), jnp.float32),
        ),
        in_specs=[smem, smem, vmem],
        out_specs=(vmem, vmem),
        name="unpack",
    )(destination, block_count, returned)
    return (grid.reshape(tiles, 3, EDGE * PLANE), new_velocity, new_affine)


def solution(mesh):
    whole = ("gx", "gy", "gz")
    return jax.shard_map(
        per_device,
        mesh=mesh,
        in_specs=(
            P(whole),
            P(None, whole),
            P(None, whole),
            P(None, whole),
            P(None, whole),
            P(whole, None),
            P(whole),
            P(whole),
            P(whole, None),
        ),
        out_specs=(P(whole, None, None), P(None, whole), P(None, whole)),
        check_vma=False,
    )
```

```python
import functools

import jax
import jax.numpy as jnp
from jax import lax
from jax.experimental import pallas as pl
from jax.experimental.pallas import tpu as pltpu
from jax.sharding import PartitionSpec as P

EDGE = 16
PLANE = EDGE * EDGE
QUANT = 1024
LANES = 128
ROWS = 80
BACK = 48
CENTER = 7.5
GROUP = 4
SMEM = pltpu.SMEM
VMEM = pltpu.VMEM


def pack_kernel(
    owner_ref, tile_ref, count_ref, mass_ref, vel_ref, aff_ref, cell_ref, frac_ref, out_ref, dest_ref, used_ref, scratch, low_ref, *, capacity, group
):
    blocks = dest_ref.shape[0]
    length = vel_ref.shape[1] // blocks
    parts = length // LANES

    def clear(owner, carry):
        used_ref[owner] = 0
        for rank in range(capacity):
            first = pl.multiple_of((owner * capacity + rank) * ROWS, 16)
            out_ref[pl.ds(first, 16), :] = jnp.full((16, LANES), -1.0, jnp.bfloat16)
        return carry

    lax.fori_loop(0, group, clear, 0)

    def place(block):
        owner = owner_ref[block]
        rank = used_ref[owner]
        used_ref[owner] = rank + 1
        slot = owner * capacity + rank
        dest_ref[block] = slot
        return slot

    place_in_block = lax.broadcasted_iota(jnp.int32, (parts, LANES), 0) * LANES
    place_in_block = place_in_block + lax.broadcasted_iota(jnp.int32, (parts, LANES), 1)

    def move(block, slot, buffer, lows):
        where = pl.ds(pl.multiple_of(block * length, LANES), length)
        code = cell_ref[:, where] * QUANT + frac_ref[:, where]
        low = (code & 127).astype(jnp.float32)
        for d in range(3):
            buffer[d : d + 1, :] = aff_ref[3 * d + 1 : 3 * d + 2, where]
            buffer[8 + d : 9 + d, :] = aff_ref[3 * d + 2 : 3 * d + 3, where]
            buffer[3 + 4 * d : 4 + 4 * d, :] = aff_ref[3 * d : 3 * d + 1, where]
        buffer[4:7, :] = vel_ref[:, where]
        buffer[12:15, :] = (code >> 7).astype(jnp.float32)
        buffer[15:16, :] = jnp.full((1, length), tile_ref[block], jnp.int32).astype(jnp.float32)
        live = jnp.where(place_in_block < count_ref[block], mass_ref[block], 0.0)
        for part in range(parts):
            lows[4 * part : 4 * part + 3, :] = low[:, part * LANES : (part + 1) * LANES]
            lows[4 * part + 3 : 4 * part + 4, :] = live[part : part + 1]
        first = pl.multiple_of(slot * ROWS, 16)
        packed = buffer[...].astype(jnp.bfloat16)
        for part in range(parts):
            out_ref[pl.ds(pl.multiple_of(first + 16 * part, 16), 16), :] = packed[:, part * LANES : (part + 1) * LANES]
        out_ref[pl.ds(pl.multiple_of(first + 16 * parts, 16), 16), :] = lows[...].astype(jnp.bfloat16)

    def step(index, carry):
        slots = [place(index * 2 + k) for k in range(2)]
        for k in range(2):
            move(index * 2 + k, slots[k], scratch.at[k], low_ref.at[k])
        return carry

    lax.fori_loop(0, blocks // 2, step, 0)


def split(value):
    high = value.astype(jnp.bfloat16)
    return high, (value - high.astype(jnp.float32)).astype(jnp.bfloat16)


def sublanes():
    return lax.broadcasted_iota(jnp.int32, (8, LANES), 0)


def spread(ref, row):
    return ref[pl.ds(row, 8, stride=0), :]


CELL, FIRST, SECOND, THIRD, MIDDLE, SIDE, NODES = (64 + 16 * k for k in range(7))
BASE = NODES + 64
TABLE = BASE + 32


def prepare(data_ref, slot, table, parts, deposit):
    first = pl.multiple_of(slot * ROWS, 16)
    side = data_ref[pl.ds(pl.multiple_of(first + 16 * parts, 16), 16), :].astype(jnp.float32)
    highs = []
    for part in range(parts):
        main = data_ref[pl.ds(pl.multiple_of(first + 16 * part, 16), 16), :].astype(jnp.float32)
        if deposit:
            table[16 * part : 16 * part + 16, :] = main
        highs.append(main[8:])
    upper = sublanes() < 4
    high = jnp.concatenate(
        [jnp.where(upper, pltpu.roll(highs[k], 4, 0), highs[k + 1]) for k in range(0, parts, 2)], axis=0
    )
    high = high * 0.125
    cell = jnp.floor(high)
    inside = (high - cell) + (side * (1.0 / QUANT) + 0.5 / QUANT)
    rest = 1.0 - inside
    table[CELL : CELL + 16, :] = cell
    table[FIRST : FIRST + 16, :] = rest * rest
    table[SECOND : SECOND + 16, :] = 1.0 + 2.0 * (inside * rest)
    table[THIRD : THIRD + 16, :] = inside * inside
    table[MIDDLE : MIDDLE + 16, :] = cell + inside + (0.5 - CENTER)
    if deposit:
        table[SIDE : SIDE + 16, :] = side * 0.125


def node_weights(table, part, e, nodes):
    row = 4 * part + e
    cell = spread(table, CELL + row)
    one, two, three = (spread(table, at + row) for at in (FIRST, SECOND, THIRD))
    return [
        jnp.where(cell == node, one, jnp.where(cell == node - 1.0, two, jnp.where(cell == node - 2.0, three, 0.0)))
        for node in nodes
    ]


def plane_table(table, part, nodes):
    for half, weight in enumerate(node_weights(table, part, 1, nodes)):
        table[NODES + 16 * part + 8 * half : NODES + 16 * part + 8 * half + 8, :] = weight
    upper, lower = node_weights(table, part, 2, nodes)
    rows = []
    for y in range(EDGE):
        weight = spread(table, NODES + 16 * part + y)
        rows.append(jnp.concatenate([weight * upper, weight * lower], axis=0).astype(jnp.bfloat16))
    return jnp.concatenate(rows, axis=0)


def node_rows():
    node = sublanes().astype(jnp.float32)
    return [node, node + 8.0]


def deposit_block(data_ref, slot, table, parts):
    prepare(data_ref, slot, table, parts, True)
    nodes = node_rows()
    leads, planes = [], []
    for part in range(parts):
        planes.append(plane_table(table, part, nodes))
        row = 4 * part
        weights = node_weights(table, part, 0, nodes)
        middle = spread(table, MIDDLE + row)
        offsets = [(node - CENTER) - middle for node in nodes]
        mass = spread(table, SIDE + row + 3)
        loaded = [mass * weight for weight in weights]
        top = table[16 * part : 16 * part + 8, :]
        bottom = table[16 * part + 8 : 16 * part + 16, :]
        base = pltpu.roll(top, 4, 0) - top * spread(table, MIDDLE + row + 1) - bottom * spread(table, MIDDLE + row + 2)
        table[BASE + 8 * part : BASE + 8 * part + 8, :] = base
        highs, lows = [jnp.concatenate(loaded, axis=0).astype(jnp.bfloat16)], []

        def add(values):
            high, low = split(jnp.concatenate(values, axis=0))
            highs.append(high)
            lows.append(low)

        for d in range(3):
            shift = spread(table, BASE + 8 * part + d)
            along_x = spread(table, 16 * part + 3 + 4 * d)
            add([load * (shift + along_x * offset) for load, offset in zip(loaded, offsets)])
        for at in (0, 8):
            for d in range(3):
                column = spread(table, 16 * part + at + d)
                add([load * column for load in loaded])
        leads.append(jnp.concatenate(highs + lows, axis=0))
    lead = jnp.concatenate(leads, axis=1)
    plane = jnp.concatenate(planes, axis=1)
    sums = lax.dot_general(lead, plane, (((1,), (1,)), ((), ())), preferred_element_type=jnp.float32)
    momentum = sums[EDGE : 10 * EDGE] + sums[10 * EDGE :]
    return jnp.concatenate([sums[:EDGE], momentum], axis=0)


def fold(values):
    row = sublanes()
    for shift in (1, 2, 4):
        if len(values) == 1:
            return values[0] + pltpu.roll(values[0], 8 - shift, 0)
        mine = (row & shift) == 0
        values = [
            jnp.where(mine, one, two) + pltpu.roll(jnp.where(mine, two, one), 8 - shift, 0)
            for one, two in zip(values[0::2], values[1::2])
        ]
    return values[0]


def interpolate_block(data_ref, grid_rows, slot, table, back_ref, parts):
    prepare(data_ref, slot, table, parts, False)
    nodes = node_rows()
    plane = jnp.concatenate([plane_table(table, part, nodes) for part in range(parts)], axis=1)
    moments = jnp.dot(grid_rows, plane, preferred_element_type=jnp.float32)
    span = 3 * EDGE
    row = sublanes()
    eights, fours = [], []
    for part in range(parts):
        weights = node_weights(table, part, 0, nodes)
        middle = spread(table, MIDDLE + 4 * part)
        offsets = [(node - CENTER) - middle for node in nodes]
        lanes = slice(part * LANES, (part + 1) * LANES)
        zero, one, two, speed = [], [], [], []
        for d in range(3):
            halves = [d * EDGE, d * EDGE + 8]
            loaded = [weight * moments[at : at + 8, lanes] for weight, at in zip(weights, halves)]
            speed.append(loaded[0] + loaded[1])
            zero.append(loaded[0] * offsets[0] + loaded[1] * offsets[1])
            for first, into in ((span, one), (3 * span, two)):
                pieces = [
                    weight * (moments[first + at : first + at + 8, lanes] + moments[first + span + at : first + span + at + 8, lanes])
                    for weight, at in zip(weights, halves)
                ]
                into.append(pieces[0] + pieces[1])
        eight = fold([zero[0], one[0], two[0], zero[1], one[1], two[1], zero[2], one[2]])
        four = fold([two[2]] + speed)
        table[BASE + 8 * part : BASE + 8 * part + 8, :] = four
        speeds = [spread(table, BASE + 8 * part + 1 + d) for d in range(3)]
        center_y = spread(table, MIDDLE + 4 * part + 1)
        center_z = spread(table, MIDDLE + 4 * part + 2)
        column = row % 3
        center = jnp.where(column == 1, center_y, jnp.where(column == 2, center_z, 0.0))
        speed = jnp.where(row < 3, speeds[0], jnp.where(row < 6, speeds[1], speeds[2]))
        eights.append(0.5 * (eight - center * speed))
        fours.append(jnp.where((row & 3) == 0, 0.5 * (four - center_z * speeds[2]), 0.125 * four))
    first = pl.multiple_of(slot * BACK, 16)
    upper = row < 4
    merged = [jnp.where(upper, fours[k], fours[k + 1]) for k in range(0, parts, 2)]
    back_ref[pl.ds(first, BACK), :] = jnp.concatenate(eights + merged, axis=0).astype(jnp.bfloat16)


def arrivals(data_ref, slots, row_ref, tile_ref, sem):
    lane = lax.broadcasted_iota(jnp.int32, (8, LANES), 1)

    def read(slot, found):
        rows = data_ref[pl.ds(pl.multiple_of(slot * ROWS, 16), 16), :].astype(jnp.float32)
        return jnp.where(lane == slot, rows[8:], found)

    found = lax.fori_loop(0, slots, read, jnp.zeros((8, LANES), jnp.float32), unroll=8)
    row_ref[...] = found.astype(jnp.int32)
    copy = pltpu.make_async_copy(row_ref, tile_ref, sem)
    copy.start()
    copy.wait()


def by_group(slots, tile_ref, work):
    def step(group, carry):
        first = group * GROUP
        many = tile_ref[7, first + GROUP // 2] >= 0

        @pl.when(many)
        def _():
            work(first, GROUP)

        @pl.when(jnp.logical_and(jnp.logical_not(many), tile_ref[7, first] >= 0))
        def _():
            work(first, GROUP // 2)

        return carry

    lax.fori_loop(0, slots // GROUP, step, 0)


def main_kernel(data_ref, drag_ref, back_ref, grid_ref, row_ref, tile_ref, sums_ref, rows_ref, table, sem, *, parts):
    tiles = drag_ref.shape[0]
    slots = data_ref.shape[0] // ROWS
    arrivals(data_ref, slots, row_ref, tile_ref, sem)

    def clear(tile, carry):
        sums_ref[tile] = jnp.zeros(sums_ref.shape[1:], jnp.float32)
        return carry

    lax.fori_loop(0, tiles, clear, 0)

    def deposit_blocks(first, count):
        sums = [deposit_block(data_ref, first + k, table.at[k], parts) for k in range(count)]
        for k in range(count):
            tile = tile_ref[7, first + k]
            tile = jnp.where(tile >= 0, tile, tiles)
            sums_ref[tile] = sums_ref[tile] + sums[k]

    by_group(slots, tile_ref, deposit_blocks)

    lane = lax.broadcasted_iota(jnp.int32, (EDGE, PLANE), 1)
    node_y = (lane >> 4).astype(jnp.float32) - CENTER
    node_z = (lane & 15).astype(jnp.float32) - CENTER

    def update(tile, carry):
        sums = sums_ref[tile]
        weight = sums[:EDGE] + drag_ref[tile]
        ones, twos, zeros = [], [], []
        for d in range(3):
            zero, one, two = (sums[EDGE * (1 + 3 * e + d) : EDGE * (2 + 3 * e + d)] for e in range(3))
            speed = (zero + node_y * one + node_z * two) / weight
            grid_ref[tile, d] = speed
            rounded = speed.astype(jnp.bfloat16)
            zeros.append(rounded)
            ones.append(split(rounded.astype(jnp.float32) * node_y))
            twos.append(split(rounded.astype(jnp.float32) * node_z))
        rows = zeros + [high for high, low in ones] + [low for high, low in ones]
        rows = rows + [high for high, low in twos] + [low for high, low in twos]
        rows_ref[tile] = jnp.concatenate(rows, axis=0)
        return carry

    lax.fori_loop(0, tiles, update, 0)

    def interpolate_blocks(first, count):
        for k in range(count):
            tile = jnp.maximum(tile_ref[7, first + k], 0)
            interpolate_block(data_ref, rows_ref[tile], first + k, table.at[k], back_ref, parts)

    by_group(slots, tile_ref, interpolate_blocks)


def unpack_kernel(dest_ref, count_ref, back_ref, vel_ref, aff_ref):
    blocks = dest_ref.shape[0]
    length = vel_ref.shape[1] // blocks
    parts = length // LANES

    def one(block):
        first = pl.multiple_of(dest_ref[block] * BACK, 16)
        rows = back_ref[pl.ds(first, BACK), :].astype(jnp.float32)
        for part in range(parts):
            lane = lax.broadcasted_iota(jnp.int32, (8, LANES), 1) + part * LANES
            present = lane < count_ref[block]
            where = pl.ds(pl.multiple_of(block * length + part * LANES, LANES), LANES)
            aff_ref[0:8, where] = jnp.where(present, rows[part * 8 : part * 8 + 8], 0.0)
            rest = jnp.where(present[:4], rows[8 * parts + part * 4 : 8 * parts + part * 4 + 4], 0.0)
            aff_ref[8:9, where] = rest[0:1]
            vel_ref[:, where] = rest[1:4]

    def step(index, carry):
        for k in range(2):
            one(index * 2 + k)
        return carry

    lax.fori_loop(0, blocks // 2, step, 0)


def per_device(
    particle_mass,
    particle_velocity,
    particle_affine,
    particle_cell,
    particle_fraction,
    block_owner,
    block_slot,
    block_count,
    cell_drag,
):
    group = lax.axis_size(("gy", "gz"))
    blocks = block_count.shape[0]
    particles = particle_mass.shape[0]
    capacity = max(1, 2 * blocks // group)
    slots = group * capacity
    tiles = cell_drag.shape[0]
    length = particles // blocks
    parts = length // LANES
    smem = pl.BlockSpec(memory_space=SMEM)
    vmem = pl.BlockSpec(memory_space=VMEM)
    outgoing, destination = pl.pallas_call(
        functools.partial(pack_kernel, capacity=capacity, group=group),
        out_shape=(
            jax.ShapeDtypeStruct((slots * ROWS, LANES), jnp.bfloat16),
            jax.ShapeDtypeStruct((blocks,), jnp.int32),
        ),
        in_specs=[smem, smem, smem, vmem, vmem, vmem, vmem, vmem],
        out_specs=(vmem, smem),
        scratch_shapes=[
            SMEM((group,), jnp.int32),
            VMEM((2, 16, length), jnp.float32),
            VMEM((2, 16, LANES), jnp.float32),
        ],
        name="pack",
    )(
        block_owner.reshape(blocks),
        block_slot,
        block_count,
        particle_mass.reshape(blocks, parts, LANES),
        particle_velocity,
        particle_affine,
        particle_cell,
        particle_fraction,
    )
    arrived = lax.all_to_all(outgoing, ("gy", "gz"), split_axis=0, concat_axis=0, tiled=True)
    span = 3 * EDGE
    back, grid = pl.pallas_call(
        functools.partial(main_kernel, parts=parts),
        out_shape=(
            jax.ShapeDtypeStruct((slots * BACK, LANES), jnp.bfloat16),
            jax.ShapeDtypeStruct((tiles, 3, EDGE, PLANE), jnp.float32),
        ),
        in_specs=[vmem, vmem],
        out_specs=(vmem, vmem),
        scratch_shapes=[
            VMEM((8, LANES), jnp.int32),
            SMEM((8, LANES), jnp.int32),
            VMEM((tiles + 1, 10 * EDGE, PLANE), jnp.float32),
            VMEM((tiles, 5 * span, PLANE), jnp.bfloat16),
            VMEM((GROUP, TABLE, LANES), jnp.float32),
            pltpu.SemaphoreType.DMA,
        ],
        name="transfer",
    )(pltpu.with_memory_space_constraint(arrived, VMEM), cell_drag.reshape(tiles, EDGE, PLANE))
    returned = lax.all_to_all(back, ("gy", "gz"), split_axis=0, concat_axis=0, tiled=True)
    new_velocity, new_affine = pl.pallas_call(
        unpack_kernel,
        out_shape=(
            jax.ShapeDtypeStruct((3, particles), jnp.float32),
            jax.ShapeDtypeStruct((9, particles), jnp.float32),
        ),
        in_specs=[smem, smem, vmem],
        out_specs=(vmem, vmem),
        name="unpack",
    )(destination, block_count, pltpu.with_memory_space_constraint(returned, VMEM))
    return (grid.reshape(tiles, 3, EDGE * PLANE), new_velocity, new_affine)


def solution(mesh):
    whole = ("gx", "gy", "gz")
    return jax.shard_map(
        per_device,
        mesh=mesh,
        in_specs=(
            P(whole),
            P(None, whole),
            P(None, whole),
            P(None, whole),
            P(None, whole),
            P(whole, None),
            P(whole),
            P(whole),
            P(whole, None),
        ),
        out_specs=(P(whole, None, None), P(None, whole), P(None, whole)),
        check_vma=False,
    )
```

```python
import functools

import jax
import jax.numpy as jnp
from jax import lax
from jax.experimental import pallas as pl
from jax.experimental.pallas import tpu as pltpu
from jax.sharding import PartitionSpec as P

EDGE = 16
PLANE = EDGE * EDGE
QUANT = 1024
LANES = 128
ROWS = 80
BACK = 48
CENTER = 7.5
DEPOSIT_GROUP = 8
INTERPOLATE_GROUP = 8
STEPS = 8
SMEM = pltpu.SMEM
VMEM = pltpu.VMEM


def pack_kernel(
    owner_ref, tile_ref, count_ref, mass_ref, vel_ref, aff_ref, cell_ref, frac_ref, out_ref, dest_ref, used_ref, scratch, low_ref, *, capacity, group
):
    blocks = dest_ref.shape[0] // STEPS
    length = vel_ref.shape[1] // blocks
    parts = length // LANES
    start = pl.program_id(0) * blocks

    def clear(owner, carry):
        used_ref[owner] = 0
        for rank in range(capacity):
            first = pl.multiple_of((owner * capacity + rank) * ROWS, 16)
            out_ref[pl.ds(first, 16), :] = jnp.full((16, LANES), -1.0, jnp.bfloat16)
        return carry

    @pl.when(start == 0)
    def _():
        lax.fori_loop(0, group, clear, 0)

    def place(block):
        owner = owner_ref[block]
        rank = used_ref[owner]
        used_ref[owner] = rank + 1
        slot = owner * capacity + rank
        dest_ref[block] = slot
        return slot

    place_in_block = lax.broadcasted_iota(jnp.int32, (parts, LANES), 0) * LANES
    place_in_block = place_in_block + lax.broadcasted_iota(jnp.int32, (parts, LANES), 1)

    def move(block, slot, buffer, lows):
        where = pl.ds(pl.multiple_of(block * length, LANES), length)
        code = cell_ref[:, where] * QUANT + frac_ref[:, where]
        low = (code & 127).astype(jnp.float32)
        for d in range(3):
            buffer[d : d + 1, :] = aff_ref[3 * d + 1 : 3 * d + 2, where]
            buffer[8 + d : 9 + d, :] = aff_ref[3 * d + 2 : 3 * d + 3, where]
            buffer[3 + 4 * d : 4 + 4 * d, :] = aff_ref[3 * d : 3 * d + 1, where]
        buffer[4:7, :] = vel_ref[:, where]
        buffer[12:15, :] = (code >> 7).astype(jnp.float32)
        buffer[15:16, :] = jnp.full((1, length), tile_ref[start + block], jnp.int32).astype(jnp.float32)
        live = jnp.where(place_in_block < count_ref[start + block], mass_ref[block], 0.0)
        for part in range(parts):
            lows[4 * part : 4 * part + 3, :] = low[:, part * LANES : (part + 1) * LANES]
            lows[4 * part + 3 : 4 * part + 4, :] = live[part : part + 1]
        first = pl.multiple_of(slot * ROWS, 16)
        packed = buffer[...].astype(jnp.bfloat16)
        for part in range(parts):
            out_ref[pl.ds(pl.multiple_of(first + 16 * part, 16), 16), :] = packed[:, part * LANES : (part + 1) * LANES]
        out_ref[pl.ds(pl.multiple_of(first + 16 * parts, 16), 16), :] = lows[...].astype(jnp.bfloat16)

    def step(index, carry):
        slots = [place(start + index * 2 + k) for k in range(2)]
        for k in range(2):
            move(index * 2 + k, slots[k], scratch.at[k], low_ref.at[k])
        return carry

    lax.fori_loop(0, blocks // 2, step, 0)


def split(value):
    high = value.astype(jnp.bfloat16)
    return high, (value - high.astype(jnp.float32)).astype(jnp.bfloat16)


def sublanes():
    return lax.broadcasted_iota(jnp.int32, (8, LANES), 0)


def spread(ref, row):
    return ref[pl.ds(row, 8, stride=0), :]


CELL, FIRST, SECOND, THIRD, SIDE = (64 + 16 * k for k in range(5))
BASE = SIDE + 16
TABLE = BASE + 32
MIDDLE = 192
KEPT = MIDDLE + 16


def prepare(data_ref, slot, table, kept, parts):
    first = pl.multiple_of(slot * ROWS, 16)
    side = data_ref[pl.ds(pl.multiple_of(first + 16 * parts, 16), 16), :].astype(jnp.float32)
    highs = []
    for part in range(parts):
        main = data_ref[pl.ds(pl.multiple_of(first + 16 * part, 16), 16), :].astype(jnp.float32)
        table[16 * part : 16 * part + 16, :] = main
        highs.append(main[8:])
    upper = sublanes() < 4
    high = jnp.concatenate(
        [jnp.where(upper, pltpu.roll(highs[k], 4, 0), highs[k + 1]) for k in range(0, parts, 2)], axis=0
    )
    high = high * 0.125
    cell = jnp.floor(high)
    inside = (high - cell) + (side * (1.0 / QUANT) + 0.5 / QUANT)
    rest = 1.0 - inside
    table[CELL : CELL + 16, :] = cell
    table[FIRST : FIRST + 16, :] = rest * rest
    table[SECOND : SECOND + 16, :] = 1.0 + 2.0 * (inside * rest)
    table[THIRD : THIRD + 16, :] = inside * inside
    table[SIDE : SIDE + 16, :] = side * 0.125
    kept[MIDDLE : MIDDLE + 16, :] = cell + inside + (0.5 - CENTER)


def node_weights(table, kept, part, e, nodes):
    row = 4 * part + e
    cell = spread(table, CELL + row)
    one, two, three = (spread(table, at + row) for at in (FIRST, SECOND, THIRD))
    weights = []
    for half, node in enumerate(nodes):
        weight = jnp.where(cell == node - 2.0, three, 0.0)
        weight = jnp.where(cell == node, one, jnp.where(cell == node - 1.0, two, weight))
        at = 64 * e + 16 * part + 8 * half
        kept[at : at + 8, :] = weight
        weights.append(weight)
    return weights


def kept_weights(kept, part, e):
    at = 64 * e + 16 * part
    return [kept[at : at + 8, :], kept[at + 8 : at + 16, :]]


def plane_table(kept, part, along_z):
    upper, lower = along_z
    rows = []
    for y in range(EDGE):
        weight = spread(kept, 64 + 16 * part + y)
        rows.append(jnp.concatenate([weight * upper, weight * lower], axis=0).astype(jnp.bfloat16))
    return jnp.concatenate(rows, axis=0)


def node_rows():
    node = sublanes().astype(jnp.float32)
    return [node, node + 8.0]


def deposit_block(data_ref, slot, table, kept, parts):
    prepare(data_ref, slot, table, kept, parts)
    nodes = node_rows()
    leads, planes = [], []
    for part in range(parts):
        node_weights(table, kept, part, 1, nodes)
        planes.append(plane_table(kept, part, node_weights(table, kept, part, 2, nodes)))
        row = 4 * part
        weights = node_weights(table, kept, part, 0, nodes)
        middle = spread(kept, MIDDLE + row)
        offsets = [(node - CENTER) - middle for node in nodes]
        mass = spread(table, SIDE + row + 3)
        loaded = [mass * weight for weight in weights]
        top = table[16 * part : 16 * part + 8, :]
        bottom = table[16 * part + 8 : 16 * part + 16, :]
        base = pltpu.roll(top, 4, 0) - top * spread(kept, MIDDLE + row + 1) - bottom * spread(kept, MIDDLE + row + 2)
        table[BASE + 8 * part : BASE + 8 * part + 8, :] = base
        highs, lows = [jnp.concatenate(loaded, axis=0).astype(jnp.bfloat16)], []

        def add(values):
            high, low = split(jnp.concatenate(values, axis=0))
            highs.append(high)
            lows.append(low)

        for d in range(3):
            shift = spread(table, BASE + 8 * part + d)
            along_x = spread(table, 16 * part + 3 + 4 * d)
            add([load * (shift + along_x * offset) for load, offset in zip(loaded, offsets)])
        for at in (0, 8):
            for d in range(3):
                column = spread(table, 16 * part + at + d)
                add([load * column for load in loaded])
        leads.append(jnp.concatenate(highs + lows, axis=0))
    lead = jnp.concatenate(leads, axis=1)
    plane = jnp.concatenate(planes, axis=1)
    sums = lax.dot_general(lead, plane, (((1,), (1,)), ((), ())), preferred_element_type=jnp.float32)
    momentum = sums[EDGE : 10 * EDGE] + sums[10 * EDGE :]
    return jnp.concatenate([sums[:EDGE], momentum], axis=0)


def fold(values):
    row = sublanes()
    for shift in (1, 2, 4):
        if len(values) == 1:
            return values[0] + pltpu.roll(values[0], 8 - shift, 0)
        mine = (row & shift) == 0
        values = [
            jnp.where(mine, one, two) + pltpu.roll(jnp.where(mine, two, one), 8 - shift, 0)
            for one, two in zip(values[0::2], values[1::2])
        ]
    return values[0]


def interpolate_block(kept, grid_rows, slot, table, back_ref, parts):
    nodes = node_rows()
    plane = jnp.concatenate([plane_table(kept, part, kept_weights(kept, part, 2)) for part in range(parts)], axis=1)
    moments = jnp.dot(grid_rows, plane, preferred_element_type=jnp.float32)
    span = 3 * EDGE
    row = sublanes()
    eights, fours = [], []
    for part in range(parts):
        weights = kept_weights(kept, part, 0)
        middle = spread(kept, MIDDLE + 4 * part)
        offsets = [(node - CENTER) - middle for node in nodes]
        lanes = slice(part * LANES, (part + 1) * LANES)
        zero, one, two, speed = [], [], [], []
        for d in range(3):
            halves = [d * EDGE, d * EDGE + 8]
            loaded = [weight * moments[at : at + 8, lanes] for weight, at in zip(weights, halves)]
            speed.append(loaded[0] + loaded[1])
            zero.append(loaded[0] * offsets[0] + loaded[1] * offsets[1])
            for first, into in ((span, one), (3 * span, two)):
                pieces = [
                    weight * (moments[first + at : first + at + 8, lanes] + moments[first + span + at : first + span + at + 8, lanes])
                    for weight, at in zip(weights, halves)
                ]
                into.append(pieces[0] + pieces[1])
        eight = fold([zero[0], one[0], two[0], zero[1], one[1], two[1], zero[2], one[2]])
        four = fold([two[2]] + speed)
        table[BASE + 8 * part : BASE + 8 * part + 8, :] = four
        speeds = [spread(table, BASE + 8 * part + 1 + d) for d in range(3)]
        center_y = spread(kept, MIDDLE + 4 * part + 1)
        center_z = spread(kept, MIDDLE + 4 * part + 2)
        column = row % 3
        center = jnp.where(column == 1, center_y, jnp.where(column == 2, center_z, 0.0))
        speed = jnp.where(row < 3, speeds[0], jnp.where(row < 6, speeds[1], speeds[2]))
        eights.append(0.5 * (eight - center * speed))
        fours.append(jnp.where((row & 3) == 0, 0.5 * (four - center_z * speeds[2]), 0.125 * four))
    first = pl.multiple_of(slot * BACK, 16)
    upper = row < 4
    merged = [jnp.where(upper, fours[k], fours[k + 1]) for k in range(0, parts, 2)]
    back_ref[pl.ds(first, BACK), :] = jnp.concatenate(eights + merged, axis=0).astype(jnp.bfloat16)


def arrivals(data_ref, slots, row_ref, tile_ref, sem):
    lane = lax.broadcasted_iota(jnp.int32, (8, LANES), 1)

    def read(slot, found):
        rows = data_ref[pl.ds(pl.multiple_of(slot * ROWS, 16), 16), :].astype(jnp.float32)
        return jnp.where(lane == slot, rows[8:], found)

    found = lax.fori_loop(0, slots, read, jnp.zeros((8, LANES), jnp.float32), unroll=8)
    row_ref[...] = found.astype(jnp.int32)
    copy = pltpu.make_async_copy(row_ref, tile_ref, sem)
    copy.start()
    copy.wait()


def by_group(slots, tile_ref, size, work):
    def step(group, carry):
        first = group * size
        many = tile_ref[7, first + 2] >= 0
        for source in range(1, size // 4):
            many = jnp.logical_and(many, tile_ref[7, first + 4 * source + 2] >= 0)

        @pl.when(many)
        def _():
            work(first, size)

        @pl.when(jnp.logical_not(many))
        def _():
            def half(index, carry):
                @pl.when(tile_ref[7, first + 2 * index] >= 0)
                def _():
                    work(first + 2 * index, 2)

                return carry

            lax.fori_loop(0, size // 2, half, 0)

        return carry

    lax.fori_loop(0, slots // size, step, 0)


def main_kernel(data_ref, drag_ref, back_ref, grid_ref, row_ref, tile_ref, sums_ref, rows_ref, table, kept_ref, sem, *, parts):
    tiles = drag_ref.shape[0]
    slots = data_ref.shape[0] // ROWS
    arrivals(data_ref, slots, row_ref, tile_ref, sem)

    def clear(tile, carry):
        sums_ref[tile] = jnp.zeros(sums_ref.shape[1:], jnp.float32)
        return carry

    lax.fori_loop(0, tiles, clear, 0)

    def deposit_blocks(first, count):
        sums = [deposit_block(data_ref, first + k, table.at[k], kept_ref.at[first + k], parts) for k in range(count)]
        for k in range(count):
            tile = tile_ref[7, first + k]
            tile = jnp.where(tile >= 0, tile, tiles)
            sums_ref[tile] = sums_ref[tile] + sums[k]

    by_group(slots, tile_ref, DEPOSIT_GROUP, deposit_blocks)

    lane = lax.broadcasted_iota(jnp.int32, (EDGE, PLANE), 1)
    node_y = (lane >> 4).astype(jnp.float32) - CENTER
    node_z = (lane & 15).astype(jnp.float32) - CENTER

    def update(tile, carry):
        sums = sums_ref[tile]
        weight = sums[:EDGE] + drag_ref[tile]
        ones, twos, zeros = [], [], []
        for d in range(3):
            zero, one, two = (sums[EDGE * (1 + 3 * e + d) : EDGE * (2 + 3 * e + d)] for e in range(3))
            speed = (zero + node_y * one + node_z * two) / weight
            grid_ref[tile, d] = speed
            rounded = speed.astype(jnp.bfloat16)
            zeros.append(rounded)
            ones.append(split(rounded.astype(jnp.float32) * node_y))
            twos.append(split(rounded.astype(jnp.float32) * node_z))
        rows = zeros + [high for high, low in ones] + [low for high, low in ones]
        rows = rows + [high for high, low in twos] + [low for high, low in twos]
        rows_ref[tile] = jnp.concatenate(rows, axis=0)
        return carry

    lax.fori_loop(0, tiles, update, 0)

    def interpolate_blocks(first, count):
        for k in range(count):
            tile = jnp.maximum(tile_ref[7, first + k], 0)
            interpolate_block(kept_ref.at[first + k], rows_ref[tile], first + k, table.at[k], back_ref, parts)

    by_group(slots, tile_ref, INTERPOLATE_GROUP, interpolate_blocks)


def unpack_kernel(dest_ref, count_ref, back_ref, vel_ref, aff_ref):
    blocks = dest_ref.shape[0] // STEPS
    length = vel_ref.shape[1] // blocks
    parts = length // LANES
    start = pl.program_id(0) * blocks

    def one(block):
        first = pl.multiple_of(dest_ref[start + block] * BACK, 16)
        rows = back_ref[pl.ds(first, BACK), :].astype(jnp.float32)
        for part in range(parts):
            lane = lax.broadcasted_iota(jnp.int32, (8, LANES), 1) + part * LANES
            present = lane < count_ref[start + block]
            where = pl.ds(pl.multiple_of(block * length + part * LANES, LANES), LANES)
            aff_ref[0:8, where] = jnp.where(present, rows[part * 8 : part * 8 + 8], 0.0)
            rest = jnp.where(present[:4], rows[8 * parts + part * 4 : 8 * parts + part * 4 + 4], 0.0)
            aff_ref[8:9, where] = rest[0:1]
            vel_ref[:, where] = rest[1:4]

    def step(index, carry):
        for k in range(2):
            one(index * 2 + k)
        return carry

    lax.fori_loop(0, blocks // 2, step, 0)


def per_device(
    particle_mass,
    particle_velocity,
    particle_affine,
    particle_cell,
    particle_fraction,
    block_owner,
    block_slot,
    block_count,
    cell_drag,
):
    group = lax.axis_size(("gy", "gz"))
    blocks = block_count.shape[0]
    particles = particle_mass.shape[0]
    capacity = max(1, 2 * blocks // group)
    slots = group * capacity
    tiles = cell_drag.shape[0]
    length = particles // blocks
    parts = length // LANES
    smem = pl.BlockSpec(memory_space=SMEM)
    vmem = pl.BlockSpec(memory_space=VMEM)

    def along(rows):
        return pl.BlockSpec((rows, particles // STEPS), lambda i: (0, i))

    outgoing, destination = pl.pallas_call(
        functools.partial(pack_kernel, capacity=capacity, group=group),
        out_shape=(
            jax.ShapeDtypeStruct((slots * ROWS, LANES), jnp.bfloat16),
            jax.ShapeDtypeStruct((blocks,), jnp.int32),
        ),
        grid=(STEPS,),
        in_specs=[
            smem,
            smem,
            smem,
            pl.BlockSpec((blocks // STEPS, parts, LANES), lambda i: (i, 0, 0)),
            along(3),
            along(9),
            along(3),
            along(3),
        ],
        out_specs=(vmem, smem),
        scratch_shapes=[
            SMEM((group,), jnp.int32),
            VMEM((2, 16, length), jnp.float32),
            VMEM((2, 16, LANES), jnp.float32),
        ],
        name="pack",
    )(
        block_owner.reshape(blocks),
        block_slot,
        block_count,
        particle_mass.reshape(blocks, parts, LANES),
        particle_velocity,
        particle_affine,
        particle_cell,
        particle_fraction,
    )
    arrived = lax.all_to_all(outgoing, ("gy", "gz"), split_axis=0, concat_axis=0, tiled=True)
    span = 3 * EDGE
    back, grid = pl.pallas_call(
        functools.partial(main_kernel, parts=parts),
        out_shape=(
            jax.ShapeDtypeStruct((slots * BACK, LANES), jnp.bfloat16),
            jax.ShapeDtypeStruct((tiles, 3, EDGE, PLANE), jnp.float32),
        ),
        in_specs=[vmem, vmem],
        out_specs=(vmem, vmem),
        scratch_shapes=[
            VMEM((8, LANES), jnp.int32),
            SMEM((8, LANES), jnp.int32),
            VMEM((tiles + 1, 10 * EDGE, PLANE), jnp.float32),
            VMEM((tiles, 5 * span, PLANE), jnp.bfloat16),
            VMEM((DEPOSIT_GROUP, TABLE, LANES), jnp.float32),
            VMEM((slots, KEPT, LANES), jnp.float32),
            pltpu.SemaphoreType.DMA,
        ],
        name="transfer",
    )(pltpu.with_memory_space_constraint(arrived, VMEM), cell_drag.reshape(tiles, EDGE, PLANE))
    returned = lax.all_to_all(back, ("gy", "gz"), split_axis=0, concat_axis=0, tiled=True)
    new_velocity, new_affine = pl.pallas_call(
        unpack_kernel,
        out_shape=(
            jax.ShapeDtypeStruct((3, particles), jnp.float32),
            jax.ShapeDtypeStruct((9, particles), jnp.float32),
        ),
        grid=(STEPS,),
        in_specs=[smem, smem, vmem],
        out_specs=(along(3), along(9)),
        name="unpack",
    )(destination, block_count, pltpu.with_memory_space_constraint(returned, VMEM))
    return (grid.reshape(tiles, 3, EDGE * PLANE), new_velocity, new_affine)


def solution(mesh):
    whole = ("gx", "gy", "gz")
    return jax.shard_map(
        per_device,
        mesh=mesh,
        in_specs=(
            P(whole),
            P(None, whole),
            P(None, whole),
            P(None, whole),
            P(None, whole),
            P(whole, None),
            P(whole),
            P(whole),
            P(whole, None),
        ),
        out_specs=(P(whole, None, None), P(None, whole), P(None, whole)),
        check_vma=False,
    )
```

```python
import functools

import jax
import jax.numpy as jnp
from jax import lax
from jax.experimental import pallas as pl
from jax.experimental.pallas import tpu as pltpu
from jax.sharding import PartitionSpec as P

EDGE = 16
PLANE = EDGE * EDGE
QUANT = 1024
LANES = 128
ROWS = 80
BACK = 48
CENTER = 7.5
DEPOSIT_GROUP = 16
INTERPOLATE_GROUP = 8
SMEM = pltpu.SMEM
VMEM = pltpu.VMEM


def pack_kernel(
    owner_ref, tile_ref, count_ref, mass_ref, vel_ref, aff_ref, cell_ref, frac_ref, out_ref, dest_ref, used_ref, scratch, low_ref, *, capacity, group
):
    blocks = dest_ref.shape[0]
    length = vel_ref.shape[1] // blocks
    parts = length // LANES

    def clear(owner, carry):
        used_ref[owner] = 0
        for rank in range(capacity):
            first = pl.multiple_of((owner * capacity + rank) * ROWS, 16)
            out_ref[pl.ds(first, 16), :] = jnp.full((16, LANES), -1.0, jnp.bfloat16)
        return carry

    lax.fori_loop(0, group, clear, 0)

    def place(block):
        owner = owner_ref[block]
        rank = used_ref[owner]
        used_ref[owner] = rank + 1
        slot = owner * capacity + rank
        dest_ref[block] = slot
        return slot

    place_in_block = lax.broadcasted_iota(jnp.int32, (parts, LANES), 0) * LANES
    place_in_block = place_in_block + lax.broadcasted_iota(jnp.int32, (parts, LANES), 1)

    def move(block, slot, buffer, lows):
        where = pl.ds(pl.multiple_of(block * length, LANES), length)
        code = cell_ref[:, where] * QUANT + frac_ref[:, where]
        low = (code & 127).astype(jnp.float32)
        for d in range(3):
            buffer[d : d + 1, :] = aff_ref[3 * d + 1 : 3 * d + 2, where]
            buffer[8 + d : 9 + d, :] = aff_ref[3 * d + 2 : 3 * d + 3, where]
            buffer[3 + 4 * d : 4 + 4 * d, :] = aff_ref[3 * d : 3 * d + 1, where]
        buffer[4:7, :] = vel_ref[:, where]
        buffer[12:15, :] = (code >> 7).astype(jnp.float32)
        buffer[15:16, :] = jnp.full((1, length), tile_ref[block], jnp.int32).astype(jnp.float32)
        live = jnp.where(place_in_block < count_ref[block], mass_ref[block], 0.0)
        for part in range(parts):
            lows[4 * part : 4 * part + 3, :] = low[:, part * LANES : (part + 1) * LANES]
            lows[4 * part + 3 : 4 * part + 4, :] = live[part : part + 1]
        first = pl.multiple_of(slot * ROWS, 16)
        packed = buffer[...].astype(jnp.bfloat16)
        for part in range(parts):
            out_ref[pl.ds(pl.multiple_of(first + 16 * part, 16), 16), :] = packed[:, part * LANES : (part + 1) * LANES]
        out_ref[pl.ds(pl.multiple_of(first + 16 * parts, 16), 16), :] = lows[...].astype(jnp.bfloat16)

    def step(index, carry):
        slots = [place(index * 4 + k) for k in range(4)]
        for k in range(4):
            move(index * 4 + k, slots[k], scratch.at[k], low_ref.at[k])
        return carry

    lax.fori_loop(0, blocks // 4, step, 0)


def split(value):
    high = value.astype(jnp.bfloat16)
    return high, (value - high.astype(jnp.float32)).astype(jnp.bfloat16)


def sublanes():
    return lax.broadcasted_iota(jnp.int32, (8, LANES), 0)


def spread(ref, row):
    return ref[pl.ds(row, 8, stride=0), :]


CELL, FIRST, SECOND, THIRD, SIDE = (64 + 16 * k for k in range(5))
BASE = SIDE + 16
TABLE = BASE + 32
MIDDLE = 192
KEPT = MIDDLE + 16


def prepare(data_ref, slot, table, kept, parts):
    first = pl.multiple_of(slot * ROWS, 16)
    side = data_ref[pl.ds(pl.multiple_of(first + 16 * parts, 16), 16), :].astype(jnp.float32)
    highs = []
    for part in range(parts):
        main = data_ref[pl.ds(pl.multiple_of(first + 16 * part, 16), 16), :].astype(jnp.float32)
        table[16 * part : 16 * part + 16, :] = main
        highs.append(main[8:])
    upper = sublanes() < 4
    high = jnp.concatenate(
        [jnp.where(upper, pltpu.roll(highs[k], 4, 0), highs[k + 1]) for k in range(0, parts, 2)], axis=0
    )
    high = high * 0.125
    cell = jnp.floor(high)
    inside = (high - cell) + (side * (1.0 / QUANT) + 0.5 / QUANT)
    rest = 1.0 - inside
    table[CELL : CELL + 16, :] = cell
    table[FIRST : FIRST + 16, :] = rest * rest
    table[SECOND : SECOND + 16, :] = 1.0 + 2.0 * (inside * rest)
    table[THIRD : THIRD + 16, :] = inside * inside
    table[SIDE : SIDE + 16, :] = side * 0.125
    kept[MIDDLE : MIDDLE + 16, :] = cell + inside + (0.5 - CENTER)


def node_weights(table, kept, part, e, nodes):
    row = 4 * part + e
    cell = spread(table, CELL + row)
    one, two, three = (spread(table, at + row) for at in (FIRST, SECOND, THIRD))
    weights = []
    for half, node in enumerate(nodes):
        weight = jnp.where(cell == node - 2.0, three, 0.0)
        weight = jnp.where(cell == node, one, jnp.where(cell == node - 1.0, two, weight))
        at = 64 * e + 16 * part + 8 * half
        kept[at : at + 8, :] = weight
        weights.append(weight)
    return weights


def kept_weights(kept, part, e):
    at = 64 * e + 16 * part
    return [kept[at : at + 8, :], kept[at + 8 : at + 16, :]]


def plane_table(kept, part, along_z):
    upper, lower = along_z
    rows = []
    for y in range(EDGE):
        weight = spread(kept, 64 + 16 * part + y)
        rows.append(jnp.concatenate([weight * upper, weight * lower], axis=0).astype(jnp.bfloat16))
    return jnp.concatenate(rows, axis=0)


def node_rows():
    node = sublanes().astype(jnp.float32)
    return [node, node + 8.0]


def deposit_block(data_ref, slot, table, kept, parts):
    prepare(data_ref, slot, table, kept, parts)
    nodes = node_rows()
    leads, planes = [], []
    for part in range(parts):
        node_weights(table, kept, part, 1, nodes)
        planes.append(plane_table(kept, part, node_weights(table, kept, part, 2, nodes)))
        row = 4 * part
        weights = node_weights(table, kept, part, 0, nodes)
        middle = spread(kept, MIDDLE + row)
        offsets = [(node - CENTER) - middle for node in nodes]
        mass = spread(table, SIDE + row + 3)
        loaded = [mass * weight for weight in weights]
        top = table[16 * part : 16 * part + 8, :]
        bottom = table[16 * part + 8 : 16 * part + 16, :]
        base = pltpu.roll(top, 4, 0) - top * spread(kept, MIDDLE + row + 1) - bottom * spread(kept, MIDDLE + row + 2)
        table[BASE + 8 * part : BASE + 8 * part + 8, :] = base
        highs, lows = [jnp.concatenate(loaded, axis=0).astype(jnp.bfloat16)], []

        def add(values):
            high, low = split(jnp.concatenate(values, axis=0))
            highs.append(high)
            lows.append(low)

        for d in range(3):
            shift = spread(table, BASE + 8 * part + d)
            along_x = spread(table, 16 * part + 3 + 4 * d)
            add([load * (shift + along_x * offset) for load, offset in zip(loaded, offsets)])
        for at in (0, 8):
            for d in range(3):
                column = spread(table, 16 * part + at + d)
                add([load * column for load in loaded])
        leads.append(jnp.concatenate(highs + lows, axis=0))
    lead = jnp.concatenate(leads, axis=1)
    plane = jnp.concatenate(planes, axis=1)
    sums = lax.dot_general(lead, plane, (((1,), (1,)), ((), ())), preferred_element_type=jnp.float32)
    momentum = sums[EDGE : 10 * EDGE] + sums[10 * EDGE :]
    return jnp.concatenate([sums[:EDGE], momentum], axis=0)


def fold(values):
    row = sublanes()
    for shift in (1, 2, 4):
        if len(values) == 1:
            return values[0] + pltpu.roll(values[0], 8 - shift, 0)
        mine = (row & shift) == 0
        values = [
            jnp.where(mine, one, two) + pltpu.roll(jnp.where(mine, two, one), 8 - shift, 0)
            for one, two in zip(values[0::2], values[1::2])
        ]
    return values[0]


def interpolate_block(kept, grid_rows, slot, table, back_ref, parts):
    nodes = node_rows()
    plane = jnp.concatenate([plane_table(kept, part, kept_weights(kept, part, 2)) for part in range(parts)], axis=1)
    moments = jnp.dot(grid_rows, plane, preferred_element_type=jnp.float32)
    span = 3 * EDGE
    row = sublanes()
    eights, fours = [], []
    for part in range(parts):
        weights = kept_weights(kept, part, 0)
        middle = spread(kept, MIDDLE + 4 * part)
        offsets = [(node - CENTER) - middle for node in nodes]
        lanes = slice(part * LANES, (part + 1) * LANES)
        zero, one, two, speed = [], [], [], []
        for d in range(3):
            halves = [d * EDGE, d * EDGE + 8]
            loaded = [weight * moments[at : at + 8, lanes] for weight, at in zip(weights, halves)]
            speed.append(loaded[0] + loaded[1])
            zero.append(loaded[0] * offsets[0] + loaded[1] * offsets[1])
            for first, into in ((span, one), (3 * span, two)):
                pieces = [
                    weight * (moments[first + at : first + at + 8, lanes] + moments[first + span + at : first + span + at + 8, lanes])
                    for weight, at in zip(weights, halves)
                ]
                into.append(pieces[0] + pieces[1])
        eight = fold([zero[0], one[0], two[0], zero[1], one[1], two[1], zero[2], one[2]])
        four = fold([two[2]] + speed)
        table[BASE + 8 * part : BASE + 8 * part + 8, :] = four
        speeds = [spread(table, BASE + 8 * part + 1 + d) for d in range(3)]
        center_y = spread(kept, MIDDLE + 4 * part + 1)
        center_z = spread(kept, MIDDLE + 4 * part + 2)
        column = row % 3
        center = jnp.where(column == 1, center_y, jnp.where(column == 2, center_z, 0.0))
        speed = jnp.where(row < 3, speeds[0], jnp.where(row < 6, speeds[1], speeds[2]))
        eights.append(0.5 * (eight - center * speed))
        fours.append(jnp.where((row & 3) == 0, 0.5 * (four - center_z * speeds[2]), 0.125 * four))
    first = pl.multiple_of(slot * BACK, 16)
    upper = row < 4
    merged = [jnp.where(upper, fours[k], fours[k + 1]) for k in range(0, parts, 2)]
    back_ref[pl.ds(first, BACK), :] = jnp.concatenate(eights + merged, axis=0).astype(jnp.bfloat16)


def arrivals(data_ref, slots, row_ref, tile_ref, sem):
    lane = lax.broadcasted_iota(jnp.int32, (8, LANES), 1)

    def read(slot, found):
        rows = data_ref[pl.ds(pl.multiple_of(slot * ROWS, 16), 16), :].astype(jnp.float32)
        return jnp.where(lane == slot, rows[8:], found)

    found = lax.fori_loop(0, slots, read, jnp.zeros((8, LANES), jnp.float32), unroll=8)
    row_ref[...] = found.astype(jnp.int32)
    copy = pltpu.make_async_copy(row_ref, tile_ref, sem)
    copy.start()
    copy.wait()


def by_group(slots, tile_ref, size, least, work):
    def step(group, carry):
        first = group * size
        filled = [tile_ref[7, first + 2 * index] >= 0 for index in range(size // 2)]
        many = sum(one.astype(jnp.int32) for one in filled) >= least

        @pl.when(many)
        def _():
            work(first, size)

        @pl.when(jnp.logical_not(many))
        def _():
            def pair(index, carry):
                @pl.when(tile_ref[7, first + 2 * index] >= 0)
                def _():
                    work(first + 2 * index, 2)

                return carry

            lax.fori_loop(0, size // 2, pair, 0)

        return carry

    lax.fori_loop(0, slots // size, step, 0)


def main_kernel(data_ref, drag_ref, back_ref, grid_ref, row_ref, tile_ref, sums_ref, rows_ref, table, kept_ref, sem, *, parts):
    tiles = drag_ref.shape[0]
    slots = data_ref.shape[0] // ROWS
    arrivals(data_ref, slots, row_ref, tile_ref, sem)

    def clear(tile, carry):
        sums_ref[tile] = jnp.zeros(sums_ref.shape[1:], jnp.float32)
        return carry

    lax.fori_loop(0, tiles, clear, 0)

    def deposit_blocks(first, count):
        sums = [deposit_block(data_ref, first + k, table.at[k], kept_ref.at[first + k], parts) for k in range(count)]
        for k in range(count):
            tile = tile_ref[7, first + k]
            tile = jnp.where(tile >= 0, tile, tiles)
            sums_ref[tile] = sums_ref[tile] + sums[k]

    by_group(slots, tile_ref, DEPOSIT_GROUP, 6, deposit_blocks)

    lane = lax.broadcasted_iota(jnp.int32, (EDGE, PLANE), 1)
    node_y = (lane >> 4).astype(jnp.float32) - CENTER
    node_z = (lane & 15).astype(jnp.float32) - CENTER

    def update(tile, carry):
        sums = sums_ref[tile]
        weight = sums[:EDGE] + drag_ref[tile]
        ones, twos, zeros = [], [], []
        for d in range(3):
            zero, one, two = (sums[EDGE * (1 + 3 * e + d) : EDGE * (2 + 3 * e + d)] for e in range(3))
            speed = (zero + node_y * one + node_z * two) / weight
            grid_ref[tile, d] = speed
            rounded = speed.astype(jnp.bfloat16)
            zeros.append(rounded)
            ones.append(split(rounded.astype(jnp.float32) * node_y))
            twos.append(split(rounded.astype(jnp.float32) * node_z))
        rows = zeros + [high for high, low in ones] + [low for high, low in ones]
        rows = rows + [high for high, low in twos] + [low for high, low in twos]
        rows_ref[tile] = jnp.concatenate(rows, axis=0)
        return carry

    lax.fori_loop(0, tiles, update, 0)

    def interpolate_blocks(first, count):
        for k in range(count):
            tile = jnp.maximum(tile_ref[7, first + k], 0)
            interpolate_block(kept_ref.at[first + k], rows_ref[tile], first + k, table.at[k], back_ref, parts)

    by_group(slots, tile_ref, INTERPOLATE_GROUP, 4, interpolate_blocks)


def unpack_kernel(dest_ref, count_ref, back_ref, vel_ref, aff_ref):
    blocks = dest_ref.shape[0]
    length = vel_ref.shape[1] // blocks
    parts = length // LANES

    def one(block):
        first = pl.multiple_of(dest_ref[block] * BACK, 16)
        rows = back_ref[pl.ds(first, BACK), :].astype(jnp.float32)
        for part in range(parts):
            lane = lax.broadcasted_iota(jnp.int32, (8, LANES), 1) + part * LANES
            present = lane < count_ref[block]
            where = pl.ds(pl.multiple_of(block * length + part * LANES, LANES), LANES)
            aff_ref[0:8, where] = jnp.where(present, rows[part * 8 : part * 8 + 8], 0.0)
            rest = jnp.where(present[:4], rows[8 * parts + part * 4 : 8 * parts + part * 4 + 4], 0.0)
            aff_ref[8:9, where] = rest[0:1]
            vel_ref[:, where] = rest[1:4]

    def step(index, carry):
        for k in range(4):
            one(index * 4 + k)
        return carry

    lax.fori_loop(0, blocks // 4, step, 0)


def per_device(
    particle_mass,
    particle_velocity,
    particle_affine,
    particle_cell,
    particle_fraction,
    block_owner,
    block_slot,
    block_count,
    cell_drag,
):
    group = lax.axis_size(("gy", "gz"))
    blocks = block_count.shape[0]
    particles = particle_mass.shape[0]
    capacity = max(1, 2 * blocks // group)
    slots = group * capacity
    tiles = cell_drag.shape[0]
    length = particles // blocks
    parts = length // LANES
    smem = pl.BlockSpec(memory_space=SMEM)
    vmem = pl.BlockSpec(memory_space=VMEM)
    outgoing, destination = pl.pallas_call(
        functools.partial(pack_kernel, capacity=capacity, group=group),
        out_shape=(
            jax.ShapeDtypeStruct((slots * ROWS, LANES), jnp.bfloat16),
            jax.ShapeDtypeStruct((blocks,), jnp.int32),
        ),
        in_specs=[smem, smem, smem, vmem, vmem, vmem, vmem, vmem],
        out_specs=(vmem, smem),
        scratch_shapes=[
            SMEM((group,), jnp.int32),
            VMEM((4, 16, length), jnp.float32),
            VMEM((4, 16, LANES), jnp.float32),
        ],
        name="pack",
    )(
        block_owner.reshape(blocks),
        block_slot,
        block_count,
        particle_mass.reshape(blocks, parts, LANES),
        particle_velocity,
        particle_affine,
        particle_cell,
        particle_fraction,
    )
    arrived = lax.all_to_all(outgoing, ("gy", "gz"), split_axis=0, concat_axis=0, tiled=True)
    span = 3 * EDGE
    back, grid = pl.pallas_call(
        functools.partial(main_kernel, parts=parts),
        out_shape=(
            jax.ShapeDtypeStruct((slots * BACK, LANES), jnp.bfloat16),
            jax.ShapeDtypeStruct((tiles, 3, EDGE, PLANE), jnp.float32),
        ),
        in_specs=[vmem, vmem],
        out_specs=(vmem, vmem),
        scratch_shapes=[
            VMEM((8, LANES), jnp.int32),
            SMEM((8, LANES), jnp.int32),
            VMEM((tiles + 1, 10 * EDGE, PLANE), jnp.float32),
            VMEM((tiles, 5 * span, PLANE), jnp.bfloat16),
            VMEM((DEPOSIT_GROUP, TABLE, LANES), jnp.float32),
            VMEM((slots, KEPT, LANES), jnp.float32),
            pltpu.SemaphoreType.DMA,
        ],
        name="transfer",
    )(pltpu.with_memory_space_constraint(arrived, VMEM), cell_drag.reshape(tiles, EDGE, PLANE))
    returned = lax.all_to_all(back, ("gy", "gz"), split_axis=0, concat_axis=0, tiled=True)
    new_velocity, new_affine = pl.pallas_call(
        unpack_kernel,
        out_shape=(
            jax.ShapeDtypeStruct((3, particles), jnp.float32),
            jax.ShapeDtypeStruct((9, particles), jnp.float32),
        ),
        in_specs=[smem, smem, vmem],
        out_specs=(vmem, vmem),
        name="unpack",
    )(destination, block_count, pltpu.with_memory_space_constraint(returned, VMEM))
    return (grid.reshape(tiles, 3, EDGE * PLANE), new_velocity, new_affine)


def solution(mesh):
    whole = ("gx", "gy", "gz")
    return jax.shard_map(
        per_device,
        mesh=mesh,
        in_specs=(
            P(whole),
            P(None, whole),
            P(None, whole),
            P(None, whole),
            P(None, whole),
            P(whole, None),
            P(whole),
            P(whole),
            P(whole, None),
        ),
        out_specs=(P(whole, None, None), P(None, whole), P(None, whole)),
        check_vma=False,
    )
```
